128 devices in a mesh: f: 4 (over x), h: 32 (over z, y, core).
Axes of the slice: x: 4, y: 4, z: 4, core: 2. Of those that a mesh axis runs over, the one named last changes fastest.
Arguments:
- x: bfloat16 [4096, 4096], P(None, 'h')
- g1: float32 [4096], P('h')
- g2: float32 [4096], P('h')
- w_gate: bfloat16 [4096, 16384], P('h', 'f')
- w_up: bfloat16 [4096, 16384], P('h', 'f')
- w_down: bfloat16 [16384, 4096], P('f', 'h')
- o: bfloat16 [4096, 4096], P(None, 'f')
- w_o: bfloat16 [4096, 4096], P('f', 'h')
- w_qkv: bfloat16 [4096, 4608], P('h', 'f')
Outputs:
- output 1: bfloat16 [4096, 4096], P(None, 'h')
- output 2: bfloat16 [4096, 4608], P(None, 'f')
All inputs are finite; a program needn't handle non-finite values.
Results may differ from the reference program's by a relative error of at most 0.00392871.
Values are sent between devices in bfloat16 or wider.
A program may use at most 1 GiB of HBM per device.

```python
import jax
import jax.numpy as jnp
from jax import lax

T = 4096
D = 4096
FF = 16384
HEADS = 16
KV_HEADS = 1
HEAD = 256
HD = HEADS * HEAD
Q = (HEADS + 2 * KV_HEADS) * HEAD
EPS = 1e-6


def _w(key, shape):
    return (jax.random.normal(key, shape, jnp.float32) * shape[0] ** -0.5).astype(jnp.bfloat16)


def setup_inputs(seed: int = 0) -> dict:
    ks = jax.random.split(jax.random.PRNGKey(seed), 11)
    z = jax.random.normal(ks[0], (T, D), jnp.float32)
    row = jnp.exp(jax.random.uniform(ks[1], (T, 1), jnp.float32, -1.0, 1.0))
    tilt = jax.random.uniform(ks[2], (T, 1), jnp.float32, -1.0, 1.0)
    pos = jnp.arange(D, dtype=jnp.float32)[None, :] * (2.0 / D) - 1.0
    x = (z * row * jnp.exp(tilt * pos)).astype(jnp.bfloat16)
    o = (0.7 * jax.random.normal(ks[8], (T, HD), jnp.float32)).astype(jnp.bfloat16)
    return {
        'x': x,
        'g1': jax.random.uniform(ks[3], (D,), jnp.float32, 0.5, 1.5),
        'g2': jax.random.uniform(ks[4], (D,), jnp.float32, 0.5, 1.5),
        'w_gate': _w(ks[5], (D, FF)),
        'w_up': _w(ks[6], (D, FF)),
        'w_down': _w(ks[7], (FF, D)),
        'o': o,
        'w_o': _w(ks[9], (HD, D)),
        'w_qkv': _w(ks[10], (D, Q)),
    }


def _norm(x, g):
    xf = x.astype(jnp.float32)
    r = lax.rsqrt(jnp.mean(xf * xf, axis=-1, keepdims=True) + EPS)
    return (xf * r * g).astype(jnp.bfloat16)


def reference(x, g1, g2, w_gate, w_up, w_down, o, w_o, w_qkv):
    n = _norm(x, g1)
    gt = jnp.dot(n, w_gate, preferred_element_type=jnp.float32)
    up = jnp.dot(n, w_up, preferred_element_type=jnp.float32)
    a = (jax.nn.silu(gt) * up).astype(jnp.bfloat16)
    y = jnp.dot(a, w_down, preferred_element_type=jnp.float32) + jnp.dot(o, w_o, preferred_element_type=jnp.float32)
    x_next = (x.astype(jnp.float32) + y).astype(jnp.bfloat16)
    n1 = _norm(x_next, g2)
    qkv = jnp.dot(n1, w_qkv, preferred_element_type=jnp.float32).astype(jnp.bfloat16)
    return (x_next, qkv)
```

```python
import jax
import jax.numpy as jnp
from jax import lax
from jax.experimental import pallas as pl
from jax.experimental.pallas import tpu as pltpu
from jax.sharding import Mesh, PartitionSpec as P

EPS = 1e-6
MESH = pl.DeviceIdType.MESH
BF = jnp.bfloat16
F32 = jnp.float32
R = 4
B = 128
H = B // 2
Q = H // 2
D = 4096
DZ = D // R
DC = DZ // 2
NQ = 4
NP = 5
PK = NP * DZ
W = 1152
NSEND, NRECV, NLOC = 24, 120, 8


def _kernel(x5, g1, g2, wg, wu, wd, o, wo, wq, xo, qo,
            XR, XN, G1S, G2S, G1F, G2F, NF, WGU, AL, AF, OB, WD, PB, RB, XP, N2, N2B, WQ, QB, ss, rs, ls):
    x, y, z, c = (lax.axis_index(a) for a in "xyzc")
    here = {"x": x, "y": y, "z": z}

    def at(axis, d):
        return lax.rem(here[axis] + d, R)

    PLUS, MINUS, FAR = 1, R - 1, 2
    oc = 1 - c
    sib = {"c": oc}
    blk = y * 2 + c

    count = {"s": 0, "r": 0, "l": 0}
    limit = {"s": NSEND, "r": NRECV, "l": NLOC}

    def new(kind):
        count[kind] += 1
        assert count[kind] <= limit[kind]
        return count[kind] - 1

    sends = []

    class Sends:
        def __init__(self, ref):
            self.i, self.ref = new("s"), ref
            sends.append(self)

        def wait(self):
            pltpu.make_async_copy(self.ref, self.ref, ss.at[self.i]).wait()

    class Got:
        def __init__(self, ref):
            self.i, self.ref = new("r"), ref

        def wait(self, ref=None):
            ref = self.ref if ref is None else ref
            pltpu.make_async_copy(ref, ref, rs.at[self.i]).wait()

    def send(group, src, dst, dev, got):
        d = pltpu.make_async_remote_copy(
            src_ref=src, dst_ref=dst, send_sem=ss.at[group.i], recv_sem=rs.at[got.i],
            device_id=dev, device_id_type=MESH)
        d.start()

    def here_copy(src, dst, got):
        pltpu.make_async_copy(src, dst, rs.at[got.i]).start()

    def load(src, dst):
        d = pltpu.make_async_copy(src, dst, ls.at[new("l")])
        d.start()
        return d

    def span(b, n):
        return pl.ds(pl.multiple_of(b * n, n), n)

    def ahead(b, n, step):
        return pl.ds(pl.multiple_of(b, step), n)

    bar = pltpu.get_barrier_semaphore()
    peers = [(dx, dy, 0, 0) for dx in range(R) for dy in range(R) if dx + dy]
    peers += [(0, dy, 0, 1) for dy in range(R)]
    peers += [(0, 0, dz, dc) for dz in range(1, R) for dc in range(2)]
    for dx, dy, dz, dc in peers:
        pl.semaphore_signal(bar, inc=1, device_id={
            "x": at("x", dx), "y": at("y", dy), "z": at("z", dz), "c": oc if dc else c}, device_id_type=MESH)

    l_ob = load(o.at[span(z * 2 + c, DC), :], OB)
    l_wd = load(wd, WD.at[z, 0:D, span(c, B)])
    l_wo = load(wo, WD.at[z, D:PK, span(c, B)])
    l_wq = load(wq, WQ.at[z, blk])
    pl.semaphore_wait(bar, len(peers))

    near = [(dy, dc) for dy in (PLUS, MINUS, FAR, 0) for dc in range(2) if dy + dc]

    def yc(dy, dc):
        return at("y", dy), (oc if dc else c)

    firsts = ((x5, XR, XN), (g1, G1S, G1F), (g2, G2S, G2F))
    s1, s1s = [Got(b) for _, b, _ in firsts], [Sends(b.at[0:R - 1]) for _, b, _ in firsts]
    for dz in (PLUS, MINUS, FAR, 0):
        z2 = at("z", dz)
        for (src, dst, _), got, grp in zip(firsts, s1, s1s):
            s = src.at[z2, :, x] if src is x5 else src
            if dz:
                send(grp, s, dst.at[z], {"z": z2}, got)
            else:
                here_copy(s, dst.at[z], got)

    a2a, a2as = [Got(WGU.at[q, span(z, DZ), :]) for q in range(NQ)], Sends(NF.at[0:NQ * 7 * 8, :])

    def send_a2a(q):
        r = span(z * 8 + blk, B)
        for dy, dc in near + [(0, 0)]:
            y2, c2 = yc(dy, dc)
            cols = span((y2 * 2 + c2) * NQ + q, B)
            for w, off in ((wg, 0), (wu, B)):
                s, d = w.at[:, cols], WGU.at[q, r, off:off + B]
                if dy + dc:
                    send(a2as, s, d, {"y": y2, "c": c2}, a2a[q])
                else:
                    here_copy(s, d, a2a[q])

    class Ring:
        def __init__(self, axis, sends, own, half):
            self.axis, self.sends, self.half = axis, sends, half
            self.got = [Got(own), Got(own)]
            self.far = [Got(half(0, 0)), Got(half(0, 1))]

        def own(self, src, dst):
            for d, g in zip((PLUS, MINUS), self.got):
                send(self.sends, src, dst, {self.axis: at(self.axis, d)}, g)

        def wait(self):
            for g in self.got:
                g.wait()

        def onward(self):
            for h, (d, g) in enumerate(zip((PLUS, MINUS), self.far)):
                ref = self.half(at(self.axis, R - d), h)
                send(self.sends, ref, ref, {self.axis: at(self.axis, d)}, g)

        def wait_far(self):
            for g in self.far:
                g.wait()

    send_a2a(0)
    qz = Ring("z", Sends(WQ.at[0, 0:R - 1]), WQ.at[0, 0], lambda zz, h: WQ.at[zz, blk, h * H:h * H + H])
    qz.own(wq, WQ.at[z, blk])

    wds, wsib = Sends(WD.at[:, 0:PK * 7 // 8, :]), {}
    cuts = [(p, p * DZ, (p + 1) * DZ) for p in range(NP)]
    wgot = [[Got(WD.at[0, s:e, 0:B]), Got(WD.at[0, s:e, 0:B])] for _, s, e in cuts]
    wsib = [Got(WD.at[0, :, 0:B]) for _ in range(3)] + [Got(WD.at[0, :, 0:B])]
    wfar = []

    def w_own(p):
        _, s, e = cuts[p]
        src, dst = (wd.at[s:e, :] if e <= D else wo), WD.at[z, s:e, span(c, B)]
        for d, g in zip((PLUS, MINUS), wgot[p]):
            send(wds, src, dst, {"z": at("z", d)}, g)
        send(wds, src, dst, sib, wsib[0])

    def w_onward(p):
        _, s, e = cuts[p]
        for h, (d, g) in enumerate(zip((PLUS, MINUS), wgot[p])):
            g.wait()
            lo, hi = max(s, h * PK // 2), min(e, (h + 1) * PK // 2)
            zz = at("z", R - d)
            if lo < hi:
                ref = WD.at[zz, lo:hi, span(c, B)]
                got = Got(ref)
                send(wds, ref, ref, {"z": at("z", d)}, got)
                wfar.append((got, lo, hi))
            ref = WD.at[zz, s:e, span(c, B)]
            send(wds, ref, ref, sib, wsib[1 + h])

    for g in s1:
        g.wait()
    less = slice(0, 7 * B)
    s2, s2s = [Got(b.at[:, :, less]) for _, _, b in firsts], [Sends(b.at[:, :, less]) for _, _, b in firsts]
    for dy, dc in near:
        y2, c2 = yc(dy, dc)
        for (_, src, dst), got, grp in zip(firsts, s2, s2s):
            send(grp, src.at[:, c2] if src is XR else src, dst.at[:, :, span(blk, B)], {"y": y2, "c": c2}, got)
    for q in range(1, NQ):
        send_a2a(q)
    XN[:, :, span(blk, B)] = XR[:, c]
    G1F[:, :, span(blk, B)] = G1S[...]
    G2F[:, :, span(blk, B)] = G2S[...]

    zs = Sends(NF.at[0:NQ * R * (R - 1) * 16, :])
    zr = [Ring("z", zs, WGU.at[q, 0:DZ, :],
               lambda zz, h, q=q: WGU.at[q, span(zz * 2 + h, DC), :]) for q in range(NQ)]

    def z_own(q):
        a2a[q].wait()
        ref = WGU.at[q, span(z, DZ), :]
        zr[q].own(ref, ref)

    def z_onward(q):
        zr[q].wait()
        zr[q].onward()

    z_own(0)
    qz.wait()
    qz.onward()

    def norm(src, gain, dst, base, first, n):
        def step(i, _):
            r = span(first // 16 + i, 16)
            v = [src[k, r, :].astype(F32) for k in range(R)]
            s = sum(jnp.sum(t * t, axis=-1, keepdims=True) for t in v)
            inv = lax.rsqrt(s / D + EPS)
            for k in range(R):
                dst[ahead(base + i * 16, 16, 16), k * DZ:(k + 1) * DZ] = (v[k] * inv * gain[k]).astype(BF)
            return 0
        lax.fori_loop(0, n // 16, step, 0)

    for g in s2:
        g.wait()
    nrow = c * R + x
    norm(XN, G1F, NF, nrow * B, 0, B)

    def nhalf(xx, h):
        return NF.at[span((c * R + xx) * 2 + h, H), :]

    ns, nsib = Sends(NF.at[0:7 * B, :]), Got(NF.at[0:DC, :])
    xr = Ring("x", ns, NF.at[0:B, :], nhalf)

    def n_sib(xx):
        ref = NF.at[span(c * R + xx, B), :]
        send(ns, ref, ref, sib, nsib)

    ref = NF.at[span(nrow, B), :]
    xr.own(ref, ref)
    n_sib(x)
    z_own(1)
    z_onward(0)
    z_own(2)
    qz.wait_far()
    l_wq.wait()
    qys, qsib = Sends(WQ.at[:, 0:7]), Got(WQ.at[:, 0:R])
    qy = Ring("y", qys, WQ.at[:, 0], lambda yy, h: WQ.at[2 * h:2 * h + 2, yy * 2 + c])

    def q_sib(yy):
        ref = WQ.at[:, yy * 2 + c]
        send(qys, ref, ref, sib, qsib)

    qy.own(WQ.at[:, blk], WQ.at[:, blk])
    q_sib(y)
    xr.wait()
    xr.onward()
    n_sib(at("x", MINUS))
    n_sib(at("x", PLUS))
    z_onward(1)
    z_own(3)
    xr.wait_far()
    n_sib(at("x", FAR))
    z_onward(2)

    one = AF.at[:, :, 0:B]
    asend = Sends(AF.at[:, :, 0:NQ * 7 * B])
    agot = [[[Got(one), Got(one)] for _ in range(2)] for _ in range(NQ)]
    arest = Got(AF.at[:, :, 0:NQ * 3 * B])

    def act(q):
        def step(m, _):
            r = span(m, 256)
            gu = jnp.dot(NF[r, :], WGU[q], preferred_element_type=F32)
            g, u = gu[:, :B], gu[:, B:]
            AL[q, r, :] = (g * lax.logistic(g) * u).astype(BF)
            return 0
        lax.fori_loop(0, R, step, 0)
        col = span(blk * NQ + q, B)
        for i, d in enumerate((PLUS, MINUS)):
            for c2 in range(2):
                for c1 in range(2):
                    @pl.when(c == c1)
                    def _():
                        send(asend, AL4.at[q, c2], AF.at[:, :, col], {"y": at("y", d), "c": c2}, agot[q][i][c1])
        send(asend, AL4.at[q, oc], AF.at[:, :, col], sib, arest)
        AF[:, :, col] = AL4[q, c]

    def a_onward(q):
        for i, d in enumerate((PLUS, MINUS)):
            agot[q][i][i].wait()
            ref = AF.at[:, :, span((at("y", R - d) * 2 + i) * NQ + q, B)]
            send(asend, ref, ref, {"y": at("y", d)}, arest)

    def a_wait():
        for q in range(NQ):
            for i in range(2):
                agot[q][i][1 - i].wait()
        arest.wait()

    AL4 = AL.reshape(NQ, 2, R, B, B)
    nsib.wait()
    zr[0].wait_far()
    act(0)
    z_onward(3)
    for p in range(NP):
        w_own(p)
    zr[1].wait_far()
    act(1)
    a_onward(0)
    zr[2].wait_far()
    act(2)
    a_onward(1)
    zr[3].wait_far()
    act(3)
    a_onward(2)
    w_onward(0)
    a_onward(3)
    qy.wait()
    qy.onward()
    q_sib(at("y", MINUS))
    q_sib(at("y", PLUS))
    w_onward(1)
    l_ob.wait()
    l_wd.wait()
    l_wo.wait()

    zk = [z, at("z", MINUS), at("z", PLUS), at("z", FAR)]
    rsend, nsend = Sends(RB), Got
    rgot = [[Got(RB.at[k, :, 0:H]) for _ in range(2)] for k in range(R)]
    ngot = [Got(N2.at[:, 0:H]) for _ in range(2)]
    xgot, xsend = [Got(xo.at[0:7 * B]), Got(xo.at[0:24 * B])], Sends(xo.at[0:31 * B])
    nsend = new("s")

    def halves(h):
        return slice(h * H, h * H + H)

    def down(k, h):
        t = halves(h)
        a, oo = AF[:, t, :].reshape(2 * B, D), OB4[:, t, :].reshape(2 * B, DZ)
        p = (jnp.dot(a, WD[zk[k], 0:D, :], preferred_element_type=F32)
             + jnp.dot(oo, WD[zk[k], D:PK, :], preferred_element_type=F32))
        PB[k, :, t, :] = p.reshape(R, H, 2 * B)
        for d in (PLUS, MINUS, FAR):
            send(rsend, PB.at[k, at("x", d), t], RB.at[k, d - 1, t], {"x": at("x", d)}, rgot[k][h])

    OB4 = OB.reshape(R, B, DZ)

    def resid(k, h):
        t = halves(h)
        rgot[k][h].wait()
        yy = PB[k, x, t] + RB[k, 0, t] + RB[k, 1, t] + RB[k, 2, t]
        cols = span(y, 2 * B)
        XP[k, t] = (XN[zk[k], t, cols].astype(F32) + yy).astype(BF)
        dst = N2.at[zk[k], t, cols]
        for d in range(R):
            cp = pltpu.make_async_remote_copy(
                src_ref=XP.at[k, t], dst_ref=dst, send_sem=ss.at[nsend], recv_sem=rs.at[ngot[h].i],
                device_id={"x": at("x", d), "y": x}, device_id_type=MESH)
            if d:
                cp.start()
            else:
                pl.when(x != y)(cp.start)

                @pl.when(x == y)
                def _():
                    dst[...] = XP[k, t]

    def x_out(k):
        rows = xo.at[span((z * 2 + c) * R + x, B), :]
        send(xsend, XP.at[k, :, span(oc, B)], rows, {"z": zk[k], "c": oc}, xgot[0])
        if k:
            send(xsend, XP.at[k, :, span(c, B)], rows, {"z": zk[k]}, xgot[0])
        else:
            rows[...] = XP[k, :, span(c, B)]

    def x_onward():
        xgot[0].wait()
        ref = xo.reshape(R, 2, R, B, B).at[:, :, x]
        for d in (PLUS, MINUS, FAR):
            send(xsend, ref, ref, {"x": at("x", d)}, xgot[1])

    wdone = [0]

    def far(n):
        for g, s, e in wfar[wdone[0]:n]:
            g.wait()
            ref = WD.at[zk[3], s:e, span(c, B)]
            send(wds, ref, ref, sib, wsib[3])
        wdone[0] = n

    a_wait()
    wsib[0].wait()
    down(0, 0)
    down(0, 1)
    w_onward(2)
    w_onward(3)
    resid(0, 0)
    resid(0, 1)
    x_out(0)
    w_onward(4)
    wsib[1].wait()
    down(1, 0)
    down(1, 1)
    far(2)
    wsib[2].wait()
    down(2, 0)
    down(2, 1)
    far(4)
    resid(1, 0)
    resid(1, 1)
    x_out(1)
    qy.wait_far()
    q_sib(at("y", FAR))
    resid(2, 0)
    resid(2, 1)
    x_out(2)
    far(len(wfar))
    wsib[3].wait()
    down(3, 0)
    down(3, 1)
    resid(3, 0)
    resid(3, 1)
    x_out(3)
    qsib.wait()

    def qrow(zz, yy, off, n):
        return qo.at[ahead(((zz * 2 + c) * R + yy) * B + off, n, Q), :]

    osend, osib = Sends(qo.at[0:31 * B]), Got(qo.at[0:D // 2])

    def qkv(h):
        t = halves(h)

        @pl.when(x == y)
        def _():
            ngot[h].wait(N2.at[:, 0:H, 0:6 * B])

        @pl.when(x != y)
        def _():
            ngot[h].wait()
        norm(N2, G2F, N2B, h * H, h * H, H)
        for j in range(3):
            cols = slice(j * 3 * B, (j + 1) * 3 * B)
            w = WQ[:, :, :, cols].reshape(D, 3 * B)
            QB[t, cols] = jnp.dot(N2B[t, :], w, preferred_element_type=F32).astype(BF)
        qo[ahead(((z * 2 + c) * R + y) * B + h * H, H, H), :] = QB[t, :]

    def out_sib(ref):
        send(osend, ref, ref, sib, osib)

    class Fan:
        def __init__(self, h):
            first, second = "yz" if h == 0 else "zy"

            def block(i, j, off, n):
                a, b = at(first, i), at(second, j)
                return qrow(b if h == 0 else a, a if h == 0 else b, h * H + off, n)

            self.block, self.first, self.second = block, first, second
            whole, part = block(0, 0, 0, H), block(0, 0, 0, Q)
            self.f, self.ff = [Got(whole), Got(whole)], [Got(part), Got(part)]
            self.s = [[Got(whole), Got(whole)] for _ in range(3)] + [[Got(part), Got(part)] for _ in range(2)]
            self.last = Got(qo.at[0:2 * B])

        def both(self, axis, ref, gots):
            for d, g in zip((PLUS, MINUS), gots):
                send(osend, ref, ref, {axis: at(axis, d)}, g)

        def go(self):
            own = self.block(0, 0, 0, H)
            self.both(self.first, own, self.f)
            self.both(self.second, own, self.s[0])
            out_sib(own)
            yield
            for i, d in enumerate((PLUS, MINUS)):
                self.f[i].wait()
                ref = self.block(R - d, 0, i * Q, Q)
                send(osend, ref, ref, {self.first: at(self.first, d)}, self.ff[i])
                ref = self.block(R - d, 0, 0, H)
                self.both(self.second, ref, self.s[1 + i])
                out_sib(ref)
            yield
            for i in range(2):
                self.ff[i].wait()
                ref = self.block(FAR, 0, i * Q, Q)
                self.both(self.second, ref, self.s[3 + i])
                out_sib(ref)
            yield
            for i, p in enumerate((0, MINUS, PLUS)):
                for u, d in enumerate((PLUS, MINUS)):
                    self.s[i][u].wait()
                    ref = self.block(p, R - d, u * Q, Q)
                    send(osend, ref, ref, {self.second: at(self.second, d)}, self.last)
                    out_sib(self.block(p, R - d, 0, H))
                yield
            for i in range(2):
                for u, d in enumerate((PLUS, MINUS)):
                    self.s[3 + i][u].wait()
                    ref = self.block(FAR, R - d, i * Q, Q)
                    if i == u:
                        send(osend, ref, ref, {self.second: at(self.second, d)}, self.last)
                    out_sib(ref)
            yield
            self.last.wait()
            for p in range(R):
                out_sib(self.block(p, FAR, 0, H))
            yield

    fans = []
    for h in range(2):
        qkv(h)
        fans.append(Fan(h).go())
        next(fans[h])
    for i, _ in enumerate(zip(*fans)):
        if i == 0:
            x_onward()
    osib.wait()
    xgot[1].wait()
    for s in sends:
        s.wait()

    @pl.when(x == y)
    def _():
        r = N2.at[:, :, 0:6 * B]
        pltpu.make_async_copy(r, r, ss.at[nsend]).wait()

    @pl.when(x != y)
    def _():
        pltpu.make_async_copy(N2, N2, ss.at[nsend]).wait()


def solution(mesh):
    mesh4 = Mesh(mesh.devices.reshape(R, R, R, 2), ("x", "z", "y", "c"))

    def body(x, g1, g2, w_gate, w_up, w_down, o, w_o, w_qkv):
        vm = pltpu.VMEM
        anyspec = pl.BlockSpec(memory_space=pl.ANY)
        sem = pltpu.SemaphoreType.DMA
        return pl.pallas_call(
            _kernel,
            out_shape=(vm((D, B), BF), vm((D, W), BF)),
            in_specs=[anyspec] * 9,
            out_specs=(pl.BlockSpec(memory_space=vm), pl.BlockSpec(memory_space=vm)),
            scratch_shapes=[
                vm((R, 2, B, B), BF),
                vm((R, B, DZ), BF),
                vm((R, 1, B), F32), vm((R, 1, B), F32),
                vm((R, 1, DZ), F32), vm((R, 1, DZ), F32),
                vm((DZ, D), BF),
                vm((NQ, D, 2 * B), BF),
                vm((NQ, DZ, B), BF),
                vm((R, B, D), BF),
                vm((DC, DZ), BF),
                vm((R, PK, 2 * B), BF),
                vm((R, R, B, 2 * B), F32),
                vm((R, R - 1, B, 2 * B), F32),
                vm((R, B, 2 * B), BF),
                vm((R, B, DZ), BF),
                vm((B, D), BF),
                vm((R, 8, B, W), BF),
                vm((B, W), BF),
                sem((NSEND,)), sem((NRECV,)), sem((NLOC,)),
            ],
            compiler_params=pltpu.CompilerParams(
                collective_id=0, has_side_effects=True, vmem_limit_bytes=50 * 2**20),
            name="block",
        )(x.reshape(R, 2, R, B, B), g1.reshape(1, B), g2.reshape(1, B), w_gate, w_up, w_down, o, w_o, w_qkv)

    h = ("z", "y", "c")
    in_specs = (P(None, h), P(h), P(h), P(h, "x"), P(h, "x"), P("x", h), P(None, "x"), P("x", h), P(h, "x"))
    return jax.shard_map(body, mesh=mesh4, in_specs=in_specs, out_specs=(P(None, h), P(None, "x")), check_vma=False)
```

```python
import jax
import jax.numpy as jnp
from jax import lax
from jax.experimental import pallas as pl
from jax.experimental.pallas import tpu as pltpu
from jax.sharding import Mesh, PartitionSpec as P

EPS = 1e-6
MESH = pl.DeviceIdType.MESH
BF = jnp.bfloat16
F32 = jnp.float32
R = 4
B = 128
H = B // 2
Q = H // 2
D = 4096
DZ = D // R
DC = DZ // 2
NQ = 4
NP = 5
PK = NP * DZ
W = 1152
NSEND, NRECV, NLOC = 24, 172, 12


def _kernel(x5, g1, g2, wg, wu, wd, o, wo, wq, xo, qo,
            XR, XN, G1S, G2S, G1F, G2F, NF, WGU, AL, AF, OB, WD, PB, RB, XP, N2, N2B, WQ, QB, ss, rs, ls):
    x, y, z, c = (lax.axis_index(a) for a in "xyzc")
    here = {"x": x, "y": y, "z": z}

    def at(axis, d):
        return lax.rem(here[axis] + d, R)

    PLUS, MINUS, FAR = 1, R - 1, 2
    oc = 1 - c
    sib = {"c": oc}
    blk = y * 2 + c

    count = {"s": 0, "r": 0, "l": 0}
    limit = {"s": NSEND, "r": NRECV, "l": NLOC}

    def new(kind):
        count[kind] += 1
        assert count[kind] <= limit[kind]
        return count[kind] - 1

    sends = []

    class Sends:
        def __init__(self, ref):
            self.i, self.ref = new("s"), ref
            sends.append(self)

        def wait(self):
            pltpu.make_async_copy(self.ref, self.ref, ss.at[self.i]).wait()

    class Got:
        def __init__(self, ref):
            self.i, self.ref = new("r"), ref

        def wait(self, ref=None):
            ref = self.ref if ref is None else ref
            pltpu.make_async_copy(ref, ref, rs.at[self.i]).wait()

    def send(group, src, dst, dev, got):
        d = pltpu.make_async_remote_copy(
            src_ref=src, dst_ref=dst, send_sem=ss.at[group.i], recv_sem=rs.at[got.i],
            device_id=dev, device_id_type=MESH)
        d.start()

    def here_copy(src, dst, got):
        pltpu.make_async_copy(src, dst, rs.at[got.i]).start()

    def load(src, dst):
        d = pltpu.make_async_copy(src, dst, ls.at[new("l")])
        d.start()
        return d

    def span(b, n):
        return pl.ds(pl.multiple_of(b * n, n), n)

    def ahead(b, n, step):
        return pl.ds(pl.multiple_of(b, step), n)

    bar = pltpu.get_barrier_semaphore()
    peers = [(dx, dy, 0, 0) for dx in range(R) for dy in range(R) if dx + dy]
    peers += [(0, dy, 0, 1) for dy in range(R)]
    peers += [(0, 0, dz, dc) for dz in range(1, R) for dc in range(2)]
    for dx, dy, dz, dc in peers:
        pl.semaphore_signal(bar, inc=1, device_id={
            "x": at("x", dx), "y": at("y", dy), "z": at("z", dz), "c": oc if dc else c}, device_id_type=MESH)

    DIST = (0, PLUS, MINUS, FAR)
    l_ob = [load(o.at[span((z * 2 + c) * R + at("x", d), B), :], OB.at[i]) for i, d in enumerate(DIST)]
    l_wd = load(wd, WD.at[z, 0:D, span(c, B)])
    l_wo = load(wo, WD.at[z, D:PK, span(c, B)])
    l_wq = load(wq, WQ.at[z, blk])
    pl.semaphore_wait(bar, len(peers))

    near = [(dy, dc) for dy in (PLUS, MINUS, FAR, 0) for dc in range(2) if dy + dc]

    def yc(dy, dc):
        return at("y", dy), (oc if dc else c)

    firsts = ((x5, XR, XN), (g1, G1S, G1F), (g2, G2S, G2F))
    s1, s1s = [Got(b) for _, b, _ in firsts], [Sends(b.at[0:R - 1]) for _, b, _ in firsts]
    for dz in (PLUS, MINUS, FAR, 0):
        z2 = at("z", dz)
        for (src, dst, _), got, grp in zip(firsts, s1, s1s):
            s = src.at[z2, :, x] if src is x5 else src
            if dz:
                send(grp, s, dst.at[z], {"z": z2}, got)
            else:
                here_copy(s, dst.at[z], got)

    a2a, a2as = [Got(WGU.at[q, span(z, DZ), :]) for q in range(NQ)], Sends(NF.at[0:NQ * 7 * 8, :])

    def send_a2a(q):
        r = span(z * 8 + blk, B)
        for dy, dc in near + [(0, 0)]:
            y2, c2 = yc(dy, dc)
            cols = span((y2 * 2 + c2) * NQ + q, B)
            for w, off in ((wg, 0), (wu, B)):
                s, d = w.at[:, cols], WGU.at[q, r, off:off + B]
                if dy + dc:
                    send(a2as, s, d, {"y": y2, "c": c2}, a2a[q])
                else:
                    here_copy(s, d, a2a[q])

    class Ring:
        def __init__(self, axis, sends, own, half):
            self.axis, self.sends, self.half = axis, sends, half
            self.got = [Got(own), Got(own)]
            self.far = [Got(half(0, 0)), Got(half(0, 1))]

        def own(self, src, dst):
            for d, g in zip((PLUS, MINUS), self.got):
                send(self.sends, src, dst, {self.axis: at(self.axis, d)}, g)

        def wait(self):
            for g in self.got:
                g.wait()

        def onward(self):
            for h, (d, g) in enumerate(zip((PLUS, MINUS), self.far)):
                ref = self.half(at(self.axis, R - d), h)
                send(self.sends, ref, ref, {self.axis: at(self.axis, d)}, g)

        def wait_far(self):
            for g in self.far:
                g.wait()

    send_a2a(0)
    send_a2a(1)
    qz = Ring("z", Sends(WQ.at[0, 0:R - 1]), WQ.at[0, 0], lambda zz, h: WQ.at[zz, blk, h * H:h * H + H])
    qz.own(wq, WQ.at[z, blk])

    wds, wsib = Sends(WD.at[:, 0:PK * 7 // 8, :]), {}
    cuts = [(p, p * DZ, (p + 1) * DZ) for p in range(NP)]
    wgot = [[Got(WD.at[0, s:e, 0:B]), Got(WD.at[0, s:e, 0:B])] for _, s, e in cuts]
    wsib = [Got(WD.at[0, :, 0:B]) for _ in range(3)] + [Got(WD.at[0, :, 0:B])]
    wfar = []

    def w_own(p):
        _, s, e = cuts[p]
        src, dst = (wd.at[s:e, :] if e <= D else wo), WD.at[z, s:e, span(c, B)]
        for d, g in zip((PLUS, MINUS), wgot[p]):
            send(wds, src, dst, {"z": at("z", d)}, g)
        send(wds, src, dst, sib, wsib[0])

    def w_onward(p):
        _, s, e = cuts[p]
        for h, (d, g) in enumerate(zip((PLUS, MINUS), wgot[p])):
            g.wait()
            lo, hi = max(s, h * PK // 2), min(e, (h + 1) * PK // 2)
            zz = at("z", R - d)
            if lo < hi:
                ref = WD.at[zz, lo:hi, span(c, B)]
                got = Got(ref)
                send(wds, ref, ref, {"z": at("z", d)}, got)
                wfar.append((got, lo, hi))
            ref = WD.at[zz, s:e, span(c, B)]
            send(wds, ref, ref, sib, wsib[1 + h])

    for g in s1:
        g.wait()
    less = slice(0, 7 * B)
    s2, s2s = [Got(b.at[:, :, less]) for _, _, b in firsts], [Sends(b.at[:, :, less]) for _, _, b in firsts]
    for dy, dc in near:
        y2, c2 = yc(dy, dc)
        for (_, src, dst), got, grp in zip(firsts, s2, s2s):
            send(grp, src.at[:, c2] if src is XR else src, dst.at[:, :, span(blk, B)], {"y": y2, "c": c2}, got)
    for q in range(2, NQ):
        send_a2a(q)
    XN[:, :, span(blk, B)] = XR[:, c]
    G1F[:, :, span(blk, B)] = G1S[...]
    G2F[:, :, span(blk, B)] = G2S[...]

    zs = Sends(NF.at[0:NQ * R * (R - 1) * 16, :])
    zr = [Ring("z", zs, WGU.at[q, 0:DZ, :],
               lambda zz, h, q=q: WGU.at[q, span(zz * 2 + h, DC), :]) for q in range(NQ)]

    def z_own(q):
        a2a[q].wait()
        ref = WGU.at[q, span(z, DZ), :]
        zr[q].own(ref, ref)

    def z_onward(q):
        zr[q].wait()
        zr[q].onward()

    z_own(0)
    z_own(1)
    qz.wait()
    qz.onward()

    def norm(src, gain, dst, base, first, n):
        def step(i, _):
            r = span(first // 16 + i, 16)
            v = [src[k, r, :].astype(F32) for k in range(R)]
            s = sum(jnp.sum(t * t, axis=-1, keepdims=True) for t in v)
            inv = lax.rsqrt(s / D + EPS)
            for k in range(R):
                dst[ahead(base + i * 16, 16, 16), k * DZ:(k + 1) * DZ] = (v[k] * inv * gain[k]).astype(BF)
            return 0
        lax.fori_loop(0, n // 16, step, 0)

    for g in s2:
        g.wait()
    nrow = c * R + x
    norm(XN, G1F, NF, nrow * B, 0, B)

    def nhalf(xx, h):
        return NF.at[span((c * R + xx) * 2 + h, H), :]

    ns, nsib = Sends(NF.at[0:7 * B, :]), [Got(NF.at[0:3 * B, :]), Got(NF.at[0:B, :])]
    xr = Ring("x", ns, NF.at[0:B, :], nhalf)

    def n_sib(xx, got):
        ref = NF.at[span(c * R + xx, B), :]
        send(ns, ref, ref, sib, got)

    ref = NF.at[span(nrow, B), :]
    xr.own(ref, ref)
    n_sib(x, nsib[0])
    z_onward(0)
    z_own(2)
    qz.wait_far()
    l_wq.wait()
    qys, qsib = Sends(WQ.at[:, 0:7]), Got(WQ.at[:, 0:R])
    qy = Ring("y", qys, WQ.at[:, 0], lambda yy, h: WQ.at[2 * h:2 * h + 2, yy * 2 + c])

    def q_sib(yy):
        ref = WQ.at[:, yy * 2 + c]
        send(qys, ref, ref, sib, qsib)

    def q_own(h):
        ref = WQ.at[2 * h:2 * h + 2, blk]
        qy.own(ref, ref)

    q_own(0)
    q_sib(y)
    z_onward(1)
    z_own(3)
    xr.wait()
    xr.onward()
    n_sib(at("x", MINUS), nsib[0])
    n_sib(at("x", PLUS), nsib[0])

    units = [[(0, 0, 3)], [(1, 0, 3)], [(0, 3, R), (1, 3, R)], [(2, 0, R)], [(3, 0, R)]]
    asend = Sends(AF.at[:, :, 0:NQ * 7 * B])
    arest = Got(AF.at[:, :, 0:NQ * 3 * B])
    agot = []
    for u in units:
        n = AF.at[0:sum(hi - lo for _, lo, hi in u), :, 0:B]
        agot.append([[Got(n), Got(n)] for _ in range(2)])
    NF4 = NF.reshape(2, R, B, D)

    def act(u):
        for q, lo, hi in units[u]:
            def step(s, _):
                xb = at("x", s + s // 2 - s // 3 * 2)
                gu = jnp.dot(NF4[:, xb].reshape(2 * B, D), WGU[q], preferred_element_type=F32)
                g, up = gu[:, :B], gu[:, B:]
                AL[q, :, s] = (g * lax.logistic(g) * up).astype(BF).reshape(2, B, B)
                return 0
            lax.fori_loop(lo, hi, step, 0)
            col = span(blk * NQ + q, B)
            dst = AF.at[lo:hi, :, col]
            for i, d in enumerate((PLUS, MINUS)):
                for c2 in range(2):
                    for c1 in range(2):
                        @pl.when(c == c1)
                        def _():
                            send(asend, AL.at[q, c2, lo:hi], dst, {"y": at("y", d), "c": c2}, agot[u][i][c1])
            send(asend, AL.at[q, oc, lo:hi], dst, sib, arest)
            AF[lo:hi, :, col] = AL[q, c, lo:hi]

    def a_onward(u):
        for i, d in enumerate((PLUS, MINUS)):
            agot[u][i][i].wait()
            for q, lo, hi in units[u]:
                ref = AF.at[lo:hi, :, span((at("y", R - d) * 2 + i) * NQ + q, B)]
                send(asend, ref, ref, {"y": at("y", d)}, arest)

    def a_wait():
        for u in range(len(units)):
            for i in range(2):
                agot[u][i][1 - i].wait()
        arest.wait()

    nsib[0].wait()
    zr[0].wait_far()
    act(0)
    z_onward(2)
    zr[1].wait_far()
    act(1)
    xr.wait_far()
    n_sib(at("x", FAR), nsib[1])
    a_onward(0)
    nsib[1].wait()
    act(2)
    a_onward(1)
    z_onward(3)
    for p in range(NP):
        w_own(p)
    a_onward(2)
    zr[2].wait_far()
    act(3)
    zr[3].wait_far()
    act(4)
    a_onward(3)
    w_onward(0)
    a_onward(4)
    q_own(1)
    w_onward(1)
    for d in l_ob:
        d.wait()
    l_wd.wait()
    l_wo.wait()

    zk = [z, at("z", MINUS), at("z", PLUS), at("z", FAR)]
    rsend, nsend = Sends(RB), Got
    rgot = [[Got(RB.at[k, :, 0:H]) for _ in range(2)] for k in range(R)]
    ngot = [Got(N2.at[:, 0:H]) for _ in range(2)]
    xgot, xsend = [Got(xo.at[0:7 * B]), Got(xo.at[0:24 * B])], Sends(xo.at[0:31 * B])
    nsend = new("s")

    def halves(h):
        return slice(h * H, h * H + H)

    def down(k, h):
        t = halves(h)
        a, oo = AF[:, t, :].reshape(2 * B, D), OB[:, t, :].reshape(2 * B, DZ)
        p = (jnp.dot(a, WD[zk[k], 0:D, :], preferred_element_type=F32)
             + jnp.dot(oo, WD[zk[k], D:PK, :], preferred_element_type=F32))
        PB[k, :, t, :] = p.reshape(R, H, 2 * B)
        for i, d in enumerate(DIST):
            if i:
                send(rsend, PB.at[k, i, t], RB.at[k, i - 1, t], {"x": at("x", d)}, rgot[k][h])

    def resid(k, h):
        t = halves(h)
        rgot[k][h].wait()
        yy = PB[k, 0, t] + RB[k, 0, t] + RB[k, 1, t] + RB[k, 2, t]
        cols = span(y, 2 * B)
        XP[k, t] = (XN[zk[k], t, cols].astype(F32) + yy).astype(BF)
        dst = N2.at[zk[k], t, cols]
        for d in range(R):
            cp = pltpu.make_async_remote_copy(
                src_ref=XP.at[k, t], dst_ref=dst, send_sem=ss.at[nsend], recv_sem=rs.at[ngot[h].i],
                device_id={"x": at("x", d), "y": x}, device_id_type=MESH)
            if d:
                cp.start()
            else:
                pl.when(x != y)(cp.start)

                @pl.when(x == y)
                def _():
                    dst[...] = XP[k, t]

    def x_out(k):
        rows = xo.at[span((z * 2 + c) * R + x, B), :]
        send(xsend, XP.at[k, :, span(oc, B)], rows, {"z": zk[k], "c": oc}, xgot[0])
        if k:
            send(xsend, XP.at[k, :, span(c, B)], rows, {"z": zk[k]}, xgot[0])
        else:
            rows[...] = XP[k, :, span(c, B)]

    def x_onward():
        xgot[0].wait()
        ref = xo.reshape(R, 2, R, B, B).at[:, :, x]
        for d in (PLUS, MINUS, FAR):
            send(xsend, ref, ref, {"x": at("x", d)}, xgot[1])

    wdone = [0]

    def far(n):
        order = [wfar[i] for t in range(len(wfar) // 2) for i in (t, t + len(wfar) // 2)]
        for g, s, e in order[wdone[0]:n]:
            g.wait()
            ref = WD.at[zk[3], s:e, span(c, B)]
            send(wds, ref, ref, sib, wsib[3])
        wdone[0] = n

    a_wait()
    wsib[0].wait()
    down(0, 0)
    down(0, 1)
    w_onward(2)
    w_onward(3)
    resid(0, 0)
    w_onward(4)
    wsib[1].wait()
    down(1, 0)
    down(1, 1)
    resid(0, 1)
    x_out(0)
    qy.wait()
    qy.onward()
    q_sib(at("y", MINUS))
    q_sib(at("y", PLUS))
    wsib[2].wait()
    down(2, 0)
    down(2, 1)
    far(2)
    resid(1, 0)
    resid(1, 1)
    x_out(1)
    far(3)
    resid(2, 0)
    far(4)
    resid(2, 1)
    x_out(2)
    far(len(wfar))
    wsib[3].wait()
    down(3, 0)
    down(3, 1)
    qy.wait_far()
    q_sib(at("y", FAR))
    resid(3, 0)
    resid(3, 1)
    x_out(3)
    qsib.wait()

    def qrow(zz, yy, off, n):
        return qo.at[ahead(((zz * 2 + c) * R + yy) * B + off, n, Q), :]

    osend, osib = Sends(qo.at[0:31 * B]), Got(qo.at[0:D // 2])

    def qkv(h):
        t = halves(h)

        @pl.when(x == y)
        def _():
            ngot[h].wait(N2.at[:, 0:H, 0:6 * B])

        @pl.when(x != y)
        def _():
            ngot[h].wait()
        norm(N2, G2F, N2B, h * H, h * H, H)
        for j in range(3):
            cols = slice(j * 3 * B, (j + 1) * 3 * B)
            w = WQ[:, :, :, cols].reshape(D, 3 * B)
            QB[t, cols] = jnp.dot(N2B[t, :], w, preferred_element_type=F32).astype(BF)
        qo[ahead(((z * 2 + c) * R + y) * B + h * H, H, H), :] = QB[t, :]

    def out_sib(ref):
        send(osend, ref, ref, sib, osib)

    todo = {}

    def coming(name, ref, then, whole):
        todo[name] = (Got(ref), then, whole)

    def fan(h):
        first, second = "yz" if h == 0 else "zy"

        def block(i, j, off, n):
            a, b = at(first, i), at(second, j)
            return qrow(b if h == 0 else a, a if h == 0 else b, h * H + off, n)

        def hop(axis, d, ref, name):
            send(osend, ref, ref, {axis: at(axis, d)}, todo[name][0])

        def across(name, i, parts):
            def start():
                for off, n, part in parts:
                    for d in (PLUS, MINUS):
                        hop(second, d, block(i, 0, off, n), f"s{h}{name}{part}{d}")
            for off, n, part in parts:
                for u, d in enumerate((PLUS, MINUS)):
                    def onward(u=u, d=d, off=off, part=part):
                        if part in ("", str(u)):
                            hop(second, d, block(i, R - d, u * Q, Q), f"l{h}{name}{u}")
                    coming(f"s{h}{name}{part}{d}", block(i, R - d, off, n), onward, block(i, R - d, off, n))
            for u in range(2):
                ref = block(i, FAR, u * Q, Q)
                coming(f"l{h}{name}{u}", ref, None, ref)
            return start

        full = [(0, H, "")]
        go = {name: across(name, i, full) for name, i in (("o", 0), ("m", MINUS), ("p", PLUS))}
        far = across("f", FAR, [(0, Q, "0"), (Q, Q, "1")])
        for u, (d, name) in enumerate(((PLUS, "m"), (MINUS, "p"))):
            def onward(u=u, d=d, name=name):
                hop(first, d, block(R - d, 0, u * Q, Q), f"r{h}{u}")
                go[name]()
            coming(f"f{h}{d}", block(R - d, 0, 0, H), onward, block(R - d, 0, 0, H))
            ref = block(FAR, 0, u * Q, Q)

            def rest(u=u):
                for d in (PLUS, MINUS):
                    hop(second, d, block(FAR, 0, u * Q, Q), f"s{h}f{u}{d}")
            coming(f"r{h}{u}", ref, rest, ref)
        own = block(0, 0, 0, H)
        for d in (PLUS, MINUS):
            hop(first, d, own, f"f{h}{d}")
        go["o"]()
        out_sib(own)

    for h in range(2):
        qkv(h)
        fan(h)
    x_onward()
    for key in "f0 s0o s1o f1 r0 s0m l1o s0p s1m l0o r1 s1p s0f0 l1m s0f1 s1f0 l0m s1f1 l0p l1p l0f l1f".split():
        for name in [n for n in todo if n.startswith(key)]:
            got, then, ref = todo.pop(name)
            got.wait()
            if then:
                then()
            out_sib(ref)
    assert not todo
    osib.wait()
    xgot[1].wait()
    for s in sends:
        s.wait()

    @pl.when(x == y)
    def _():
        r = N2.at[:, :, 0:6 * B]
        pltpu.make_async_copy(r, r, ss.at[nsend]).wait()

    @pl.when(x != y)
    def _():
        pltpu.make_async_copy(N2, N2, ss.at[nsend]).wait()


def solution(mesh):
    mesh4 = Mesh(mesh.devices.reshape(R, R, R, 2), ("x", "z", "y", "c"))

    def body(x, g1, g2, w_gate, w_up, w_down, o, w_o, w_qkv):
        vm = pltpu.VMEM
        anyspec = pl.BlockSpec(memory_space=pl.ANY)
        sem = pltpu.SemaphoreType.DMA
        return pl.pallas_call(
            _kernel,
            out_shape=(vm((D, B), BF), vm((D, W), BF)),
            in_specs=[anyspec] * 9,
            out_specs=(pl.BlockSpec(memory_space=vm), pl.BlockSpec(memory_space=vm)),
            scratch_shapes=[
                vm((R, 2, B, B), BF),
                vm((R, B, DZ), BF),
                vm((R, 1, B), F32), vm((R, 1, B), F32),
                vm((R, 1, DZ), F32), vm((R, 1, DZ), F32),
                vm((DZ, D), BF),
                vm((NQ, D, 2 * B), BF),
                vm((NQ, 2, R, B, B), BF),
                vm((R, B, D), BF),
                vm((R, B, DZ), BF),
                vm((R, PK, 2 * B), BF),
                vm((R, R, B, 2 * B), F32),
                vm((R, R - 1, B, 2 * B), F32),
                vm((R, B, 2 * B), BF),
                vm((R, B, DZ), BF),
                vm((B, D), BF),
                vm((R, 8, B, W), BF),
                vm((B, W), BF),
                sem((NSEND,)), sem((NRECV,)), sem((NLOC,)),
            ],
            compiler_params=pltpu.CompilerParams(
                collective_id=0, has_side_effects=True, vmem_limit_bytes=50 * 2**20),
            name="block",
        )(x.reshape(R, 2, R, B, B), g1.reshape(1, B), g2.reshape(1, B), w_gate, w_up, w_down, o, w_o, w_qkv)

    h = ("z", "y", "c")
    in_specs = (P(None, h), P(h), P(h), P(h, "x"), P(h, "x"), P("x", h), P(None, "x"), P("x", h), P(h, "x"))
    return jax.shard_map(body, mesh=mesh4, in_specs=in_specs, out_specs=(P(None, h), P(None, "x")), check_vma=False)
```

```python
import jax
import jax.numpy as jnp
from jax import lax
from jax.experimental import pallas as pl
from jax.experimental.pallas import tpu as pltpu
from jax.sharding import Mesh, PartitionSpec as P

EPS = 1e-6
MESH = pl.DeviceIdType.MESH
BF = jnp.bfloat16
F32 = jnp.float32
R = 4
B = 128
H = B // 2
Q = H // 2
D = 4096
DZ = D // R
DC = DZ // 2
NQ = 4
NP = 4
W = 1152
NSEND, NRECV, NLOC = 30, 200, 20


def _kernel(x5, g1, g2, wg, wu, wd, o, wo, wq, xo, qo,
            XR, XN, G1S, G2S, G1F, G2F, NF, WGU, AL, AF, OT, WO, OR, OS, OD, WD, PB, RB, XP, N2, N2B, WQ,
            ss, rs, ls):
    x, y, z, c = (lax.axis_index(a) for a in "xyzc")
    here = {"x": x, "y": y, "z": z}

    def at(axis, d):
        return lax.rem(here[axis] + d, R)

    PLUS, MINUS, FAR = 1, R - 1, 2
    oc = 1 - c
    sib = {"c": oc}
    blk = y * 2 + c

    count = {"s": 0, "r": 0, "l": 0}
    limit = {"s": NSEND, "r": NRECV, "l": NLOC}

    def new(kind):
        count[kind] += 1
        assert count[kind] <= limit[kind]
        return count[kind] - 1

    sends = []

    class Sends:
        def __init__(self, ref):
            self.i, self.ref = new("s"), ref
            sends.append(self)

        def wait(self):
            pltpu.make_async_copy(self.ref, self.ref, ss.at[self.i]).wait()

    class Got:
        def __init__(self, ref):
            self.i, self.ref = new("r"), ref

        def wait(self, ref=None):
            ref = self.ref if ref is None else ref
            pltpu.make_async_copy(ref, ref, rs.at[self.i]).wait()

    def send(group, src, dst, dev, got):
        d = pltpu.make_async_remote_copy(
            src_ref=src, dst_ref=dst, send_sem=ss.at[group.i], recv_sem=rs.at[got.i],
            device_id=dev, device_id_type=MESH)
        d.start()

    def here_copy(src, dst, got):
        pltpu.make_async_copy(src, dst, rs.at[got.i]).start()

    def load(src, dst):
        d = pltpu.make_async_copy(src, dst, ls.at[new("l")])
        d.start()
        return d

    def span(b, n):
        return pl.ds(pl.multiple_of(b * n, n), n)

    def ahead(b, n, step):
        return pl.ds(pl.multiple_of(b, step), n)

    bar = pltpu.get_barrier_semaphore()
    peers = [(dx, dy, 0, 0) for dx in range(R) for dy in range(R) if dx + dy]
    peers += [(0, dy, 0, 1) for dy in range(R)]
    peers += [(0, 0, dz, dc) for dz in range(1, R) for dc in range(2)]
    for dx, dy, dz, dc in peers:
        pl.semaphore_signal(bar, inc=1, device_id={
            "x": at("x", dx), "y": at("y", dy), "z": at("z", dz), "c": oc if dc else c}, device_id_type=MESH)

    DIST = (0, PLUS, MINUS, FAR)
    l_wo = load(wo, WO)
    NT = D // (2 * B)
    tiles = [pltpu.make_async_copy(o.at[i * 2 * B:(i + 1) * 2 * B, :], OT.at[i % R], ls.at[new("l")]) for i in range(NT)]
    for i in range(R):
        tiles[i].start()
    l_wd = load(wd, WD.at[z, :, span(c, B)])
    l_wq = load(wq, WQ.at[z, blk])
    pl.semaphore_wait(bar, len(peers))

    near = [(dy, dc) for dy in (PLUS, MINUS, FAR, 0) for dc in range(2) if dy + dc]

    def yc(dy, dc):
        return at("y", dy), (oc if dc else c)

    firsts = ((x5, XR, XN), (g1, G1S, G1F), (g2, G2S, G2F))
    s1, s1s = [Got(b) for _, b, _ in firsts], [Sends(b.at[0:R - 1]) for _, b, _ in firsts]
    for dz in (PLUS, MINUS, FAR, 0):
        z2 = at("z", dz)
        for (src, dst, _), got, grp in zip(firsts, s1, s1s):
            s = src.at[z2, :, x] if src is x5 else src
            if dz:
                send(grp, s, dst.at[z], {"z": z2}, got)
            else:
                here_copy(s, dst.at[z], got)

    a2a, a2as = [Got(WGU.at[q, span(z, DZ), :]) for q in range(NQ)], Sends(NF.at[0:NQ * 7 * 8, :])

    def send_a2a(q):
        r = span(z * 8 + blk, B)
        for dy, dc in near + [(0, 0)]:
            y2, c2 = yc(dy, dc)
            cols = span((y2 * 2 + c2) * NQ + q, B)
            for w, off in ((wg, 0), (wu, B)):
                s, d = w.at[:, cols], WGU.at[q, r, off:off + B]
                if dy + dc:
                    send(a2as, s, d, {"y": y2, "c": c2}, a2a[q])
                else:
                    here_copy(s, d, a2a[q])

    class Ring:
        def __init__(self, axis, sends, own, half):
            self.axis, self.sends, self.half = axis, sends, half
            self.got = [Got(own), Got(own)]
            self.far = [Got(half(0, 0)), Got(half(0, 1))]

        def own(self, src, dst):
            for d, g in zip((PLUS, MINUS), self.got):
                send(self.sends, src, dst, {self.axis: at(self.axis, d)}, g)

        def wait(self):
            for g in self.got:
                g.wait()

        def onward(self):
            for h, (d, g) in enumerate(zip((PLUS, MINUS), self.far)):
                ref = self.half(at(self.axis, R - d), h)
                send(self.sends, ref, ref, {self.axis: at(self.axis, d)}, g)

        def wait_far(self):
            for g in self.far:
                g.wait()

    send_a2a(0)
    send_a2a(1)
    qz = Ring("z", Sends(WQ.at[0, 0:R - 1]), WQ.at[0, 0], lambda zz, h: WQ.at[zz, blk, h * H:h * H + H])
    qz.own(wq, WQ.at[z, blk])

    wds = Sends(WD.at[:, 0:D * 7 // 8, :])
    cuts = [(p, p * DZ, (p + 1) * DZ) for p in range(NP)]
    wgot = [[Got(WD.at[0, s:e, 0:B]), Got(WD.at[0, s:e, 0:B])] for _, s, e in cuts]
    wsib = [Got(WD.at[0, :, 0:B]) for _ in range(3)] + [Got(WD.at[0, :, 0:B])]
    wfar = []

    def w_own(p):
        _, s, e = cuts[p]
        src, dst = wd.at[s:e, :], WD.at[z, s:e, span(c, B)]
        for d, g in zip((PLUS, MINUS), wgot[p]):
            send(wds, src, dst, {"z": at("z", d)}, g)
        send(wds, src, dst, sib, wsib[0])

    def w_onward(p):
        _, s, e = cuts[p]
        for h, (d, g) in enumerate(zip((PLUS, MINUS), wgot[p])):
            g.wait()
            lo, hi = max(s, h * D // 2), min(e, (h + 1) * D // 2)
            zz = at("z", R - d)
            if lo < hi:
                ref = WD.at[zz, lo:hi, span(c, B)]
                got = Got(ref)
                send(wds, ref, ref, {"z": at("z", d)}, got)
                wfar.append((got, lo, hi))
            ref = WD.at[zz, s:e, span(c, B)]
            send(wds, ref, ref, sib, wsib[1 + h])

    l_wo.wait()
    os, og = Sends(OR), Got(OR)
    for i in range(NT):
        tiles[i].wait()
        p, q, r = i // 2 // 2, i // 2 % 2, i % 2 * 2
        PB[p, q, r:r + 2] = jnp.dot(OT[i % R], WO[...], preferred_element_type=F32).reshape(2, B, B)
        if i + R < NT:
            tiles[i + R].start()
        if q and r:
            for j, d in enumerate((PLUS, MINUS, FAR)):
                send(os, PB.at[p, :, at("x", d)], OR.at[j, p], {"x": at("x", d)}, og)
    for g in s1:
        g.wait()
    less = slice(0, 7 * B)
    s2, s2s = [Got(b.at[:, :, less]) for _, _, b in firsts], [Sends(b.at[:, :, less]) for _, _, b in firsts]
    for dy, dc in near:
        y2, c2 = yc(dy, dc)
        for (_, src, dst), got, grp in zip(firsts, s2, s2s):
            send(grp, src.at[:, c2] if src is XR else src, dst.at[:, :, span(blk, B)], {"y": y2, "c": c2}, got)
    for q in range(2, NQ):
        send_a2a(q)
    XN[:, :, span(blk, B)] = XR[:, c]
    G1F[:, :, span(blk, B)] = G1S[...]
    G2F[:, :, span(blk, B)] = G2S[...]

    zs = Sends(NF.at[0:NQ * R * (R - 1) * 16, :])
    zr = [Ring("z", zs, WGU.at[q, 0:DZ, :],
               lambda zz, h, q=q: WGU.at[q, span(zz * 2 + h, DC), :]) for q in range(NQ)]

    def z_own(q):
        a2a[q].wait()
        ref = WGU.at[q, span(z, DZ), :]
        zr[q].own(ref, ref)

    def z_onward(q):
        zr[q].wait()
        zr[q].onward()

    z_own(0)
    z_own(1)
    qz.wait()
    qz.onward()

    def norm(src, gain, dst, base, first, n):
        def step(i, _):
            r = span(first // 16 + i, 16)
            v = [src[k, r, :].astype(F32) for k in range(R)]
            s = sum(jnp.sum(t * t, axis=-1, keepdims=True) for t in v)
            inv = lax.rsqrt(s / D + EPS)
            for k in range(R):
                dst[ahead(base + i * 16, 16, 16), k * DZ:(k + 1) * DZ] = (v[k] * inv * gain[k]).astype(BF)
            return 0
        lax.fori_loop(0, n // 16, step, 0)

    for g in s2:
        g.wait()
    nrow = c * R + x
    norm(XN, G1F, NF, nrow * B, 0, B)

    def nhalf(xx, h):
        return NF.at[span((c * R + xx) * 2 + h, H), :]

    ns, nsib = Sends(NF.at[0:7 * B, :]), [Got(NF.at[0:3 * B, :]), Got(NF.at[0:B, :])]
    xr = Ring("x", ns, NF.at[0:B, :], nhalf)

    def n_sib(xx, got):
        ref = NF.at[span(c * R + xx, B), :]
        send(ns, ref, ref, sib, got)

    ref = NF.at[span(nrow, B), :]
    xr.own(ref, ref)
    n_sib(x, nsib[0])
    z_onward(0)
    z_own(2)
    qz.wait_far()
    l_wq.wait()
    qys, qsib = Sends(WQ.at[:, 0:7]), Got(WQ.at[:, 0:R])
    slab = WQ.at[0, 0]
    qgot = [[Got(slab), Got(slab)] for _ in range(R)]
    qfar = [Got(slab) for _ in range(R)]

    def q_own(j):
        ref = WQ.at[j, blk]
        for d, g in zip((PLUS, MINUS), qgot[j]):
            send(qys, ref, ref, {"y": at("y", d)}, g)
        send(qys, ref, ref, sib, qsib)

    def q_onward(j):
        for i, (d, g) in enumerate(zip((PLUS, MINUS), qgot[j])):
            g.wait()
            ref = WQ.at[j, at("y", R - d) * 2 + c]
            if i == j // 2:
                send(qys, ref, ref, {"y": at("y", d)}, qfar[j])
            send(qys, ref, ref, sib, qsib)

    def q_last(j):
        qfar[j].wait()
        ref = WQ.at[j, at("y", FAR) * 2 + c]
        send(qys, ref, ref, sib, qsib)

    for j in (0, 2, 1):
        q_own(j)
    z_onward(1)
    z_own(3)
    xr.wait()
    xr.onward()
    n_sib(at("x", MINUS), nsib[0])
    n_sib(at("x", PLUS), nsib[0])

    og.wait()
    OS[...] = PB[:, :, x] + OR[0] + OR[1] + OR[2]
    zs2, zg2 = Sends(OD.at[0:R - 1]), Got(OD.at[0:R - 1])
    os.wait()
    sends.remove(os)

    def o_send():
        for dc in range(2):
            c2 = oc if dc else c
            for d in (PLUS, MINUS, FAR):
                send(zs2, OS.at[at("z", d), c2], OD.at[z, :, span(c, B)], {"z": at("z", d), "c": c2}, zg2)
        send(os2, OS.at[z, oc], OD.at[z, :, span(c, B)], sib, og2)
        OD[z, :, span(c, B)] = OS[z, c]

    os2, og2 = Sends(OD.at[0, :, 0:B]), Got(OD.at[0, :, 0:B])

    units = [[(0, 0, 3)], [(1, 0, 3)], [(0, 3, R), (1, 3, R)], [(2, 0, R)], [(3, 0, R)]]
    asend = Sends(AF.at[:, :, 0:NQ * 7 * B])
    arest = Got(AF.at[:, :, 0:NQ * 3 * B])
    agot = []
    for u in units:
        n = AF.at[0:sum(hi - lo for _, lo, hi in u), :, 0:B]
        agot.append([[Got(n), Got(n)] for _ in range(2)])
    NF4 = NF.reshape(2, R, B, D)

    def act(u):
        for q, lo, hi in units[u]:
            def step(s, _):
                xb = at("x", s + s // 2 - s // 3 * 2)
                gu = jnp.dot(NF4[:, xb].reshape(2 * B, D), WGU[q], preferred_element_type=F32)
                g, up = gu[:, :B], gu[:, B:]
                AL[q, :, s] = (g * lax.logistic(g) * up).astype(BF).reshape(2, B, B)
                return 0
            lax.fori_loop(lo, hi, step, 0)
            col = span(blk * NQ + q, B)
            dst = AF.at[lo:hi, :, col]
            for i, d in enumerate((PLUS, MINUS)):
                for c2 in range(2):
                    for c1 in range(2):
                        @pl.when(c == c1)
                        def _():
                            send(asend, AL.at[q, c2, lo:hi], dst, {"y": at("y", d), "c": c2}, agot[u][i][c1])
            send(asend, AL.at[q, oc, lo:hi], dst, sib, arest)
            AF[lo:hi, :, col] = AL[q, c, lo:hi]

    def a_onward(u):
        for i, d in enumerate((PLUS, MINUS)):
            agot[u][i][i].wait()
            for q, lo, hi in units[u]:
                ref = AF.at[lo:hi, :, span((at("y", R - d) * 2 + i) * NQ + q, B)]
                send(asend, ref, ref, {"y": at("y", d)}, arest)

    def a_wait():
        for u in range(len(units)):
            for i in range(2):
                agot[u][i][1 - i].wait()
        arest.wait()

    nsib[0].wait()
    zr[0].wait_far()
    act(0)
    z_onward(2)
    zr[1].wait_far()
    act(1)
    xr.wait_far()
    n_sib(at("x", FAR), nsib[1])
    a_onward(0)
    nsib[1].wait()
    act(2)
    a_onward(1)
    z_onward(3)
    q_onward(0)
    q_onward(2)
    for p in range(NP):
        w_own(p)
    o_send()
    a_onward(2)
    zr[2].wait_far()
    act(3)
    zr[3].wait_far()
    act(4)
    a_onward(3)
    w_onward(0)
    a_onward(4)
    q_own(3)
    q_onward(1)
    w_onward(1)
    l_wd.wait()

    zk = [z, at("z", MINUS), at("z", PLUS), at("z", FAR)]
    rsend = [Sends(RB.at[0:R - 1]), Sends(RB.at[0])]
    block = RB.at[0, 0, 0, 0:H]
    rgot = [[Got(RB.at[k, :, :, 0:H]) if k == R - 1 else [Got(block), Got(block), Got(RB.at[k, 0:2, :, 0:H])]
             for _ in range(2)] for k in range(R)]
    ngot = [Got(N2.at[:, 0:H]) for _ in range(2)]
    xgot, xsend = [Got(xo.at[0:7 * B]), Got(xo.at[0:24 * B])], Sends(xo.at[0:31 * B])
    nsend = new("s")

    def halves(h):
        return slice(h * H, h * H + H)

    def down(k, h):
        t = halves(h)
        p = jnp.dot(AF[:, t, :].reshape(2 * B, D), WD[zk[k]], preferred_element_type=F32)
        for i in range(2):
            PB[k, i, :, t] = p[:, i * B:(i + 1) * B].reshape(R, H, B)
        if k == R - 1:
            for i, d in enumerate(DIST):
                if i:
                    send(rsend[1], PB.at[k, :, i, t], RB.at[k, i - 1, :, t], {"x": at("x", d)}, rgot[k][h])
            return
        for i, d in enumerate((PLUS, MINUS)):
            to = {"x": at("x", d)}
            send(rsend[0], PB.at[k, i, R - 1, t], RB.at[k, R - 2, i, t], to, rgot[k][h][i])
            send(rsend[0], PB.at[k, 1 - i, 1 + i, t], RB.at[k, i, 1 - i, t], to, rgot[k][h][2])

    def add(k, h):
        t = halves(h)
        for i, d in enumerate((PLUS, MINUS)):
            rgot[k][h][i].wait()
            PB[k, i, 1 + i, t] = PB[k, i, 1 + i, t] + RB[k, R - 2, i, t]
            send(rsend[0], PB.at[k, i, 1 + i, t], RB.at[k, i, i, t], {"x": at("x", d)}, rgot[k][h][2])

    def resid(k, h):
        t = halves(h)
        (rgot[k][h] if k == R - 1 else rgot[k][h][2]).wait()
        cols = span(y, 2 * B)
        for i in range(2):
            part = slice(i * B, (i + 1) * B)
            yy = OD[zk[k], t, part] + PB[k, i, 0, t] + RB[k, 0, i, t] + RB[k, 1, i, t]
            if k == R - 1:
                yy = yy + RB[k, 2, i, t]
            XP[k, t, part] = (XN[zk[k], t, span(y * 2 + i, B)].astype(F32) + yy).astype(BF)
        dst = N2.at[zk[k], t, cols]
        for d in range(R):
            cp = pltpu.make_async_remote_copy(
                src_ref=XP.at[k, t], dst_ref=dst, send_sem=ss.at[nsend], recv_sem=rs.at[ngot[h].i],
                device_id={"x": at("x", d), "y": x}, device_id_type=MESH)
            if d:
                cp.start()
            else:
                pl.when(x != y)(cp.start)

                @pl.when(x == y)
                def _():
                    dst[...] = XP[k, t]

    def x_out(k):
        rows = xo.at[span((z * 2 + c) * R + x, B), :]
        send(xsend, XP.at[k, :, span(oc, B)], rows, {"z": zk[k], "c": oc}, xgot[0])
        if k:
            send(xsend, XP.at[k, :, span(c, B)], rows, {"z": zk[k]}, xgot[0])
        else:
            rows[...] = XP[k, :, span(c, B)]

    def x_onward():
        xgot[0].wait()
        ref = xo.reshape(R, 2, R, B, B).at[:, :, x]
        for d in (PLUS, MINUS, FAR):
            send(xsend, ref, ref, {"x": at("x", d)}, xgot[1])

    wdone = [0]

    def far(n):
        order = [wfar[i] for t in range(len(wfar) // 2) for i in (t, t + len(wfar) // 2)]
        for g, s, e in order[wdone[0]:n]:
            g.wait()
            ref = WD.at[zk[3], s:e, span(c, B)]
            send(wds, ref, ref, sib, wsib[3])
        wdone[0] = n

    a_wait()
    wsib[0].wait()
    down(0, 0)
    down(0, 1)
    w_onward(2)
    w_onward(3)
    wsib[1].wait()
    add(0, 0)
    down(1, 0)
    add(0, 1)
    down(1, 1)
    wsib[2].wait()
    down(2, 0)
    add(1, 0)
    down(2, 1)
    add(1, 1)
    og2.wait()
    zg2.wait()
    resid(0, 0)
    resid(0, 1)
    x_out(0)
    q_onward(3)
    q_last(0)
    q_last(2)
    add(2, 0)
    resid(1, 0)
    add(2, 1)
    resid(1, 1)
    x_out(1)
    far(2)
    resid(2, 0)
    far(len(wfar))
    resid(2, 1)
    x_out(2)
    wsib[3].wait()
    down(3, 0)
    down(3, 1)
    resid(3, 0)
    q_last(1)
    q_last(3)
    resid(3, 1)
    x_out(3)
    qsib.wait()

    def qrow(zz, yy, off, n):
        return qo.at[ahead(((zz * 2 + c) * R + yy) * B + off, n, Q), :]

    osend, osib = Sends(qo.at[0:31 * B]), Got(qo.at[0:D // 2])

    def qkv(h):
        t = halves(h)

        @pl.when(x == y)
        def _():
            ngot[h].wait(N2.at[:, 0:H, 0:6 * B])

        @pl.when(x != y)
        def _():
            ngot[h].wait()
        norm(N2, G2F, N2B, h * H, h * H, H)
        for j in range(3):
            cols = slice(j * 3 * B, (j + 1) * 3 * B)
            w = WQ[:, :, :, cols].reshape(D, 3 * B)
            qo[ahead(((z * 2 + c) * R + y) * B + h * H, H, H), cols] = jnp.dot(
                N2B[t, :], w, preferred_element_type=F32).astype(BF)
            fan[h](cols)

    def out_sib(ref):
        send(osend, ref, ref, sib, osib)

    todo = {}

    def coming(name, ref, then, whole):
        todo[name] = (Got(ref), then, whole)

    def arrivals(h):
        first, second = "yz" if h == 0 else "zy"

        def block(i, j, off, n):
            a, b = at(first, i), at(second, j)
            return qrow(b if h == 0 else a, a if h == 0 else b, h * H + off, n)

        def hop(axis, d, ref, name):
            send(osend, ref, ref, {axis: at(axis, d)}, todo[name][0])

        def across(name, i, parts):
            def start():
                for off, n, part in parts:
                    for d in (PLUS, MINUS):
                        hop(second, d, block(i, 0, off, n), f"s{h}{name}{part}{d}")
            for off, n, part in parts:
                for u, d in enumerate((PLUS, MINUS)):
                    def onward(u=u, d=d, off=off, part=part):
                        if part in ("", str(u)):
                            hop(second, d, block(i, R - d, u * Q, Q), f"l{h}{name}{u}")
                    coming(f"s{h}{name}{part}{d}", block(i, R - d, off, n), onward, block(i, R - d, off, n))
            for u in range(2):
                ref = block(i, FAR, u * Q, Q)
                coming(f"l{h}{name}{u}", ref, None, ref)
            return start

        full = [(0, H, "")]
        go = {name: across(name, i, full) for name, i in (("o", 0), ("m", MINUS), ("p", PLUS))}
        across("f", FAR, [(0, Q, "0"), (Q, Q, "1")])
        for u, (d, name) in enumerate(((PLUS, "m"), (MINUS, "p"))):
            def onward(u=u, d=d, name=name):
                hop(first, d, block(R - d, 0, u * Q, Q), f"r{h}{u}")
                go[name]()
            coming(f"f{h}{d}", block(R - d, 0, 0, H), onward, block(R - d, 0, 0, H))
            ref = block(FAR, 0, u * Q, Q)

            def rest(u=u):
                for d in (PLUS, MINUS):
                    hop(second, d, block(FAR, 0, u * Q, Q), f"s{h}f{u}{d}")
            coming(f"r{h}{u}", ref, rest, ref)

        def own(cols):
            ref = block(0, 0, 0, H).at[:, cols]
            for d in (PLUS, MINUS):
                hop(first, d, ref, f"f{h}{d}")
            for d in (PLUS, MINUS):
                hop(second, d, ref, f"s{h}o{d}")
            out_sib(ref)
        return own

    fan = [arrivals(h) for h in range(2)]
    for h in range(2):
        qkv(h)
    x_onward()
    for key in ("f0", "s0o", "s1o", "f1", "r0", "s0m", "l1o", "s0p", "s1m", "l0o", "r1", "s1p",
                "s0f0", "l1m", "s0f1", "s1f0", "l0m", "s1f1", "l0p", "l1p", "l0f", "l1f"):
        for name in [n for n in todo if n.startswith(key)]:
            got, then, ref = todo.pop(name)
            got.wait()
            if then:
                then()
            out_sib(ref)
    assert not todo
    osib.wait()
    xgot[1].wait()
    for s in sends:
        s.wait()

    @pl.when(x == y)
    def _():
        r = N2.at[:, :, 0:6 * B]
        pltpu.make_async_copy(r, r, ss.at[nsend]).wait()

    @pl.when(x != y)
    def _():
        pltpu.make_async_copy(N2, N2, ss.at[nsend]).wait()


def _copy(a, b, c, d, sem):
    n = 4
    cps = []
    for i, (src, dst) in enumerate(((a, c), (b, d))):
        for j in range(n):
            r = slice(j * D // n, (j + 1) * D // n)
            cps.append(pltpu.make_async_copy(src.at[r], dst.at[r], sem.at[i, j]))
            cps[-1].start()
    for cp in cps:
        cp.wait()


def solution(mesh):
    mesh4 = Mesh(mesh.devices.reshape(R, R, R, 2), ("x", "z", "y", "c"))

    def body(x, g1, g2, w_gate, w_up, w_down, o, w_o, w_qkv):
        vm = pltpu.VMEM
        anyspec = pl.BlockSpec(memory_space=pl.ANY)
        sem = pltpu.SemaphoreType.DMA
        outs = pl.pallas_call(
            _kernel,
            out_shape=(vm((D, B), BF), vm((D, W), BF)),
            in_specs=[anyspec] * 9,
            out_specs=(pl.BlockSpec(memory_space=vm), pl.BlockSpec(memory_space=vm)),
            scratch_shapes=[
                vm((R, 2, B, B), BF),
                vm((R, B, DZ), BF),
                vm((R, 1, B), F32), vm((R, 1, B), F32),
                vm((R, 1, DZ), F32), vm((R, 1, DZ), F32),
                vm((DZ, D), BF),
                vm((NQ, D, 2 * B), BF),
                vm((NQ, 2, R, B, B), BF),
                vm((R, B, D), BF),
                vm((R, 2 * B, DZ), BF),
                vm((DZ, B), BF),
                vm((R - 1, R, 2, B, B), F32),
                vm((R, 2, B, B), F32),
                vm((R, B, 2 * B), F32),
                vm((R, D, 2 * B), BF),
                vm((R, 2, R, B, B), F32),
                vm((R, R - 1, 2, B, B), F32),
                vm((R, B, 2 * B), BF),
                vm((R, B, DZ), BF),
                vm((B, D), BF),
                vm((R, 8, B, W), BF),
                sem((NSEND,)), sem((NRECV,)), sem((NLOC,)),
            ],
            compiler_params=pltpu.CompilerParams(
                collective_id=0, has_side_effects=True, vmem_limit_bytes=53 * 2**20),
            name="block",
        )(x.reshape(R, 2, R, B, B), g1.reshape(1, B), g2.reshape(1, B), w_gate, w_up, w_down, o, w_o, w_qkv)
        return pl.pallas_call(
            _copy,
            out_shape=(jax.ShapeDtypeStruct((D, B), BF), jax.ShapeDtypeStruct((D, W), BF)),
            in_specs=[pl.BlockSpec(memory_space=vm)] * 2,
            out_specs=(anyspec, anyspec),
            scratch_shapes=[sem((2, 4))],
            compiler_params=pltpu.CompilerParams(vmem_limit_bytes=2**20),
            name="store",
        )(*outs)

    h = ("z", "y", "c")
    in_specs = (P(None, h), P(h), P(h), P(h, "x"), P(h, "x"), P("x", h), P(None, "x"), P("x", h), P(h, "x"))
    return jax.shard_map(body, mesh=mesh4, in_specs=in_specs, out_specs=(P(None, h), P(None, "x")), check_vma=False)
```

```python
import jax
import jax.numpy as jnp
from jax import lax
from jax.experimental import pallas as pl
from jax.experimental.pallas import tpu as pltpu
from jax.sharding import Mesh, PartitionSpec as P

EPS = 1e-6
MESH = pl.DeviceIdType.MESH
BF = jnp.bfloat16
F32 = jnp.float32
R = 4
B = 128
H = B // 2
Q = H // 2
D = 4096
DZ = D // R
DC = DZ // 2
NQ = 4
NP = 4
W = 1152
NSEND, NRECV, NLOC = 30, 216, 20


def _kernel(x5, g1, g2, wg, wu, wd, o, wo, wq, xo, qo,
            XR, XN, G1S, G2S, G1F, G2F, NF, WGU, AL, AF, OT, WO, OR, OS, OD, WD, PB, RB, XP, N2, N2B, WQ,
            ss, rs, ls):
    x, y, z, c = (lax.axis_index(a) for a in "xyzc")
    here = {"x": x, "y": y, "z": z}

    def at(axis, d):
        return lax.rem(here[axis] + d, R)

    PLUS, MINUS, FAR = 1, R - 1, 2
    oc = 1 - c
    sib = {"c": oc}
    blk = y * 2 + c

    count = {"s": 0, "r": 0, "l": 0}
    limit = {"s": NSEND, "r": NRECV, "l": NLOC}

    def new(kind):
        count[kind] += 1
        assert count[kind] <= limit[kind]
        return count[kind] - 1

    sends = []

    class Sends:
        def __init__(self, ref):
            self.i, self.ref = new("s"), ref
            sends.append(self)

        def wait(self):
            pltpu.make_async_copy(self.ref, self.ref, ss.at[self.i]).wait()

    class Got:
        def __init__(self, ref):
            self.i, self.ref = new("r"), ref

        def wait(self, ref=None):
            ref = self.ref if ref is None else ref
            pltpu.make_async_copy(ref, ref, rs.at[self.i]).wait()

    def send(group, src, dst, dev, got):
        d = pltpu.make_async_remote_copy(
            src_ref=src, dst_ref=dst, send_sem=ss.at[group.i], recv_sem=rs.at[got.i],
            device_id=dev, device_id_type=MESH)
        d.start()

    def here_copy(src, dst, got):
        pltpu.make_async_copy(src, dst, rs.at[got.i]).start()

    def load(src, dst):
        d = pltpu.make_async_copy(src, dst, ls.at[new("l")])
        d.start()
        return d

    def span(b, n):
        return pl.ds(pl.multiple_of(b * n, n), n)

    def ahead(b, n, step):
        return pl.ds(pl.multiple_of(b, step), n)

    bar = pltpu.get_barrier_semaphore()
    peers = [(dx, 0, 0, 0) for dx in range(1, R)]
    peers += [(0, dy, 0, dc) for dy in range(R) for dc in range(2) if dy + dc]
    peers += [(0, 0, dz, dc) for dz in range(1, R) for dc in range(2)]
    for dx, dy, dz, dc in peers:
        pl.semaphore_signal(bar, inc=1, device_id={
            "x": at("x", dx), "y": at("y", dy), "z": at("z", dz), "c": oc if dc else c}, device_id_type=MESH)

    DIST = (0, PLUS, MINUS, FAR)
    l_wo = load(wo, WO)
    NT = D // (2 * B)
    tiles = [pltpu.make_async_copy(o.at[i * 2 * B:(i + 1) * 2 * B, :], OT.at[i % R], ls.at[new("l")]) for i in range(NT)]
    for i in range(R):
        tiles[i].start()
    l_wd = load(wd, WD.at[z, :, span(c, B)])
    l_wq = load(wq, WQ.at[z, blk])
    pl.semaphore_wait(bar, len(peers))

    near = [(dy, dc) for dy in (PLUS, MINUS, FAR, 0) for dc in range(2) if dy + dc]

    def yc(dy, dc):
        return at("y", dy), (oc if dc else c)

    firsts = ((x5, XR, XN), (g1, G1S, G1F), (g2, G2S, G2F))
    s1, s1s = [Got(b) for _, b, _ in firsts], [Sends(b.at[0:R - 1]) for _, b, _ in firsts]
    for dz in (PLUS, MINUS, FAR, 0):
        z2 = at("z", dz)
        for (src, dst, _), got, grp in zip(firsts, s1, s1s):
            s = src.at[z2, :, x] if src is x5 else src
            if dz:
                send(grp, s, dst.at[z], {"z": z2}, got)
            else:
                here_copy(s, dst.at[z], got)

    a2a, a2as = [Got(WGU.at[q, span(z, DZ), :]) for q in range(NQ)], Sends(NF.at[0:NQ * 7 * 8, :])

    def send_a2a(q):
        r = span(z * 8 + blk, B)
        for dy, dc in near + [(0, 0)]:
            y2, c2 = yc(dy, dc)
            cols = span((y2 * 2 + c2) * NQ + q, B)
            for w, off in ((wg, 0), (wu, B)):
                s, d = w.at[:, cols], WGU.at[q, r, off:off + B]
                if dy + dc:
                    send(a2as, s, d, {"y": y2, "c": c2}, a2a[q])
                else:
                    here_copy(s, d, a2a[q])

    class Ring:
        def __init__(self, axis, sends, own, half):
            self.axis, self.sends, self.half = axis, sends, half
            self.got = [Got(own), Got(own)]
            self.far = [Got(half(0, 0)), Got(half(0, 1))]

        def own(self, src, dst):
            for d, g in zip((PLUS, MINUS), self.got):
                send(self.sends, src, dst, {self.axis: at(self.axis, d)}, g)

        def wait(self):
            for g in self.got:
                g.wait()

        def onward(self):
            for h, (d, g) in enumerate(zip((PLUS, MINUS), self.far)):
                ref = self.half(at(self.axis, R - d), h)
                send(self.sends, ref, ref, {self.axis: at(self.axis, d)}, g)

        def wait_far(self):
            for g in self.far:
                g.wait()

    send_a2a(0)
    send_a2a(1)
    qz = Ring("z", Sends(WQ.at[0, 0:R - 1]), WQ.at[0, 0], lambda zz, h: WQ.at[zz, blk, h * H:h * H + H])
    qz.own(wq, WQ.at[z, blk])

    wds = Sends(WD.at[:, 0:D * 7 // 8, :])
    cuts = [(p, p * DZ, (p + 1) * DZ) for p in range(NP)]
    wgot = [[Got(WD.at[0, s:e, 0:B]), Got(WD.at[0, s:e, 0:B])] for _, s, e in cuts]
    piece = WD.at[0, 0:DZ, 0:B]
    wsib, wnear = Got(WD.at[0, :, 0:B]), [[Got(piece), Got(piece)] for _ in range(NP)]
    wfar, wlast = [[Got(piece), Got(piece)] for _ in range(2)], [Got(WD.at[0, 0:2 * DZ, 0:B]) for _ in range(2)]

    def cut(i, h):
        p = (i + 2 * h) % NP
        return cuts[p]

    def w_own(i):
        for h, (d, g) in enumerate(zip((PLUS, MINUS), wgot[i])):
            _, s, e = cut(i, h)
            send(wds, wd.at[s:e, :], WD.at[z, s:e, span(c, B)], {"z": at("z", d)}, g)
        _, s, e = cuts[i]
        send(wds, wd.at[s:e, :], WD.at[z, s:e, span(c, B)], sib, wsib)

    def w_onward(i):
        for h, (d, g) in enumerate(zip((PLUS, MINUS), wgot[i])):
            g.wait()
            _, s, e = cut(i, h)
            ref = WD.at[at("z", R - d), s:e, span(c, B)]
            send(wds, ref, ref, sib, wnear[i][h])

    def w_near(h, ps):
        for p in ps:
            wnear[p][h].wait()

    def w_far(h, lane):
        d = (PLUS, MINUS)[h]
        ref = WD.at[at("z", R - d), span(2 * h + c, DZ), lane * B:(lane + 1) * B]
        send(wds, ref, ref, {"z": at("z", d)}, wfar[lane][h])

    def far(lane):
        for h, g in enumerate(wfar[lane]):
            g.wait()
            ref = WD.at[at("z", FAR), span(2 * h + c, DZ), lane * B:(lane + 1) * B]
            send(wds, ref, ref, sib, wlast[lane])

    l_wo.wait()
    os, og = Sends(OR), Got(OR)
    for i in range(NT):
        tiles[i].wait()
        p, q, r = i // 2 // 2, i // 2 % 2, i % 2 * 2
        PB[p, q, r:r + 2] = jnp.dot(OT[i % R], WO[...], preferred_element_type=F32).reshape(2, B, B)
        if i + R < NT:
            tiles[i + R].start()
        if q and r:
            for j, d in enumerate((PLUS, MINUS, FAR)):
                send(os, PB.at[p, :, at("x", d)], OR.at[j, p], {"x": at("x", d)}, og)
    for g in s1:
        g.wait()
    less = slice(0, 7 * B)
    s2, s2s = [Got(b.at[:, :, less]) for _, _, b in firsts], [Sends(b.at[:, :, less]) for _, _, b in firsts]
    for dy, dc in near:
        y2, c2 = yc(dy, dc)
        for (_, src, dst), got, grp in zip(firsts, s2, s2s):
            send(grp, src.at[:, c2] if src is XR else src, dst.at[:, :, span(blk, B)], {"y": y2, "c": c2}, got)
    for q in range(2, NQ):
        send_a2a(q)
    XN[:, :, span(blk, B)] = XR[:, c]
    G1F[:, :, span(blk, B)] = G1S[...]
    G2F[:, :, span(blk, B)] = G2S[...]

    zs = Sends(NF.at[0:NQ * R * (R - 1) * 16, :])
    zr = [Ring("z", zs, WGU.at[q, 0:DZ, :],
               lambda zz, h, q=q: WGU.at[q, span(zz * 2 + h, DC), :]) for q in range(NQ)]

    def z_own(q):
        a2a[q].wait()
        ref = WGU.at[q, span(z, DZ), :]
        zr[q].own(ref, ref)

    def z_onward(q):
        zr[q].wait()
        zr[q].onward()

    z_own(0)
    z_own(1)
    qz.wait()
    qz.onward()

    def norm(src, gain, dst, base, first, n):
        def step(i, _):
            r = span(first // 16 + i, 16)
            v = [src[k, r, :].astype(F32) for k in range(R)]
            s = sum(jnp.sum(t * t, axis=-1, keepdims=True) for t in v)
            inv = lax.rsqrt(s / D + EPS)
            for k in range(R):
                dst[ahead(base + i * 16, 16, 16), k * DZ:(k + 1) * DZ] = (v[k] * inv * gain[k]).astype(BF)
            return 0
        lax.fori_loop(0, n // 16, step, 0)

    for g in s2:
        g.wait()
    nrow = c * R + x
    norm(XN, G1F, NF, nrow * B, 0, B)

    def nhalf(xx, h):
        return NF.at[span((c * R + xx) * 2 + h, H), :]

    ns, nsib = Sends(NF.at[0:7 * B, :]), [Got(NF.at[0:3 * B, :]), Got(NF.at[0:B, :])]
    xr = Ring("x", ns, NF.at[0:B, :], nhalf)

    def n_sib(xx, got):
        ref = NF.at[span(c * R + xx, B), :]
        send(ns, ref, ref, sib, got)

    ref = NF.at[span(nrow, B), :]
    xr.own(ref, ref)
    n_sib(x, nsib[0])
    z_onward(0)
    z_own(2)
    qz.wait_far()
    l_wq.wait()
    qys, qsib = Sends(WQ.at[:, 0:7]), Got(WQ.at[:, 0:R])
    slab = WQ.at[0, 0]
    qgot = [[Got(slab), Got(slab)] for _ in range(R)]
    qfar = [Got(slab) for _ in range(R)]

    def q_own(j):
        ref = WQ.at[j, blk]
        for d, g in zip((PLUS, MINUS), qgot[j]):
            send(qys, ref, ref, {"y": at("y", d)}, g)
        send(qys, ref, ref, sib, qsib)

    def q_onward(j):
        for i, (d, g) in enumerate(zip((PLUS, MINUS), qgot[j])):
            g.wait()
            ref = WQ.at[j, at("y", R - d) * 2 + c]
            if i == j // 2:
                send(qys, ref, ref, {"y": at("y", d)}, qfar[j])
            send(qys, ref, ref, sib, qsib)

    def q_last(j):
        qfar[j].wait()
        ref = WQ.at[j, at("y", FAR) * 2 + c]
        send(qys, ref, ref, sib, qsib)

    for j in (0, 2, 1):
        q_own(j)
    z_onward(1)
    z_own(3)
    xr.wait()
    xr.onward()
    n_sib(at("x", MINUS), nsib[0])
    n_sib(at("x", PLUS), nsib[0])

    og.wait()
    OS[...] = PB[:, :, x] + OR[0] + OR[1] + OR[2]
    zs2, zg2 = Sends(OD.at[0:R - 1]), [Got(OD.at[0:2]), Got(OD.at[0])]
    os2, og2 = Sends(OD.at[0, :, 0:B]), Got(OD.at[0, :, 0:B])
    os.wait()
    sends.remove(os)

    def o_send(ds, got):
        for d in ds:
            for c2 in (c, oc):
                send(zs2, OS.at[at("z", d), c2], OD.at[z, :, span(c, B)], {"z": at("z", d), "c": c2}, got)

    units = [[(0, 0, 3)], [(1, 0, 3)], [(0, 3, R), (1, 3, R)], [(2, 0, 2)], [(2, 2, R)], [(3, 0, 2)], [(3, 2, R)]]
    asend = Sends(AF.at[:, :, 0:NQ * 7 * B])
    arest = Got(AF.at[:, :, 0:NQ * 3 * B])
    agot = []
    for u in units:
        n = AF.at[0:sum(hi - lo for _, lo, hi in u), :, 0:B]
        agot.append([[Got(n), Got(n)] for _ in range(2)])
    NF4 = NF.reshape(2, R, B, D)

    def act(u):
        for q, lo, hi in units[u]:
            def step(s, _):
                xb = at("x", s + s // 2 - s // 3 * 2)
                gu = jnp.dot(NF4[:, xb].reshape(2 * B, D), WGU[q], preferred_element_type=F32)
                g, up = gu[:, :B], gu[:, B:]
                AL[q, :, s] = (g * lax.logistic(g) * up).astype(BF).reshape(2, B, B)
                return 0
            lax.fori_loop(lo, hi, step, 0)
            col = span(blk * NQ + q, B)
            dst = AF.at[lo:hi, :, col]
            for i, d in enumerate((PLUS, MINUS)):
                for c2 in range(2):
                    for c1 in range(2):
                        @pl.when(c == c1)
                        def _():
                            send(asend, AL.at[q, c2, lo:hi], dst, {"y": at("y", d), "c": c2}, agot[u][i][c1])
            send(asend, AL.at[q, oc, lo:hi], dst, sib, arest)
            AF[lo:hi, :, col] = AL[q, c, lo:hi]

    def a_onward(u):
        for i, d in enumerate((PLUS, MINUS)):
            agot[u][i][i].wait()
            for q, lo, hi in units[u]:
                ref = AF.at[lo:hi, :, span((at("y", R - d) * 2 + i) * NQ + q, B)]
                send(asend, ref, ref, {"y": at("y", d)}, arest)

    def a_wait():
        for u in range(len(units)):
            for i in range(2):
                agot[u][i][1 - i].wait()
        arest.wait()

    nsib[0].wait()
    zr[0].wait_far()
    act(0)
    z_onward(2)
    zr[1].wait_far()
    act(1)
    xr.wait_far()
    n_sib(at("x", FAR), nsib[1])
    a_onward(0)
    nsib[1].wait()
    act(2)
    a_onward(1)
    z_onward(3)
    q_onward(0)
    q_onward(2)
    for p in range(NP):
        w_own(p)
    o_send((PLUS, MINUS), zg2[0])
    send(os2, OS.at[z, oc], OD.at[z, :, span(c, B)], sib, og2)
    OD[z, :, span(c, B)] = OS[z, c]
    a_onward(2)
    zr[2].wait_far()
    act(3)
    act(4)
    zr[3].wait_far()
    act(5)
    act(6)
    a_onward(3)
    a_onward(4)
    w_onward(0)
    a_onward(5)
    a_onward(6)
    q_own(3)
    q_onward(1)
    w_onward(1)
    l_wd.wait()

    zk = [z, at("z", MINUS), at("z", PLUS), at("z", FAR)]
    rsend = [Sends(RB.at[0:R - 1]), Sends(RB.at[0])]
    block = RB.at[0, 0, 0, 0:H]
    rgot = [[[Got(block), Got(block), Got(RB.at[k, 0:2, :, 0:H])] for _ in range(2)] for k in range(R - 1)]
    rlast = [[Got(RB.at[0, :, 0, 0:H]) for _ in range(2)] for _ in range(2)]
    ngot = [Got(N2.at[:, 0:H]) for _ in range(2)]
    xgot, xsend = [Got(xo.at[0:7 * B]), Got(xo.at[0:24 * B])], Sends(xo.at[0:31 * B])
    nsend = new("s")

    def halves(h):
        return slice(h * H, h * H + H)

    def product(k, h, w, kk=slice(0, D)):
        return jnp.dot(AF[:, halves(h), kk].reshape(2 * B, w.shape[0]), w, preferred_element_type=F32)

    def early(k, h):
        spans = [slice(0, D - DZ)] if k == 1 else [slice(2 * DZ, D), slice(0, DZ)]
        p = sum(product(k, h, WD[zk[k], kk], kk) for kk in spans)
        for i in range(2):
            PB[k, i, :, halves(h)] = p[:, i * B:(i + 1) * B].reshape(R, H, B)

    def down_last(i, h):
        t, k = halves(h), R - 1
        p = product(k, h, WD[zk[k], :, i * B:(i + 1) * B])
        PB[k, i, :, t] = p.reshape(R, H, B)
        for j, d in enumerate(DIST):
            if j:
                send(rsend[1], PB.at[k, i, j, t], RB.at[k, j - 1, i, t], {"x": at("x", d)}, rlast[i][h])

    def down(k, h):
        t = halves(h)
        kk = (slice(0, D), slice(D - DZ, D), slice(DZ, 2 * DZ))[k]
        p = product(k, h, WD[zk[k], kk], kk)
        for i in range(2):
            v = p[:, i * B:(i + 1) * B].reshape(R, H, B)
            PB[k, i, :, t] = PB[k, i, :, t] + v if k else v
        for i, d in enumerate((PLUS, MINUS)):
            to = {"x": at("x", d)}
            send(rsend[0], PB.at[k, i, R - 1, t], RB.at[k, R - 2, i, t], to, rgot[k][h][i])
            send(rsend[0], PB.at[k, 1 - i, 1 + i, t], RB.at[k, i, 1 - i, t], to, rgot[k][h][2])

    def add(k, h):
        t = halves(h)
        for i, d in enumerate((PLUS, MINUS)):
            rgot[k][h][i].wait()
            PB[k, i, 1 + i, t] = PB[k, i, 1 + i, t] + RB[k, R - 2, i, t]
            send(rsend[0], PB.at[k, i, 1 + i, t], RB.at[k, i, i, t], {"x": at("x", d)}, rgot[k][h][2])

    def finish(k, h, i, yy):
        t, part = halves(h), slice(i * B, (i + 1) * B)
        XP[k, t, part] = (XN[zk[k], t, span(y * 2 + i, B)].astype(F32) + (OD[zk[k], t, part] + PB[k, i, 0, t] + yy)).astype(BF)

    def resid(k, h):
        t = halves(h)
        rgot[k][h][2].wait()
        for i in range(2):
            finish(k, h, i, RB[k, 0, i, t] + RB[k, 1, i, t])

    def resid_last(i, h):
        t, k = halves(h), R - 1
        rlast[i][h].wait()
        finish(k, h, i, RB[k, 0, i, t] + RB[k, 1, i, t] + RB[k, 2, i, t])

    def tell(k, h, i=None):
        t = halves(h)
        if i is None:
            src, dst = XP.at[k, t], N2.at[zk[k], t, span(y, 2 * B)]
        else:
            src, dst = XP.at[k, t, i * B:(i + 1) * B], N2.at[zk[k], t, span(y * 2 + i, B)]
        for d in range(R):
            cp = pltpu.make_async_remote_copy(
                src_ref=src, dst_ref=dst, send_sem=ss.at[nsend], recv_sem=rs.at[ngot[h].i],
                device_id={"x": at("x", d), "y": x}, device_id_type=MESH)
            if d:
                cp.start()
            else:
                pl.when(x != y)(cp.start)

                @pl.when(x == y)
                def _():
                    dst[...] = src[...]

    def x_out(k):
        rows = xo.at[span((z * 2 + c) * R + x, B), :]
        send(xsend, XP.at[k, :, span(oc, B)], rows, {"z": zk[k], "c": oc}, xgot[0])
        if k:
            send(xsend, XP.at[k, :, span(c, B)], rows, {"z": zk[k]}, xgot[0])
        else:
            rows[...] = XP[k, :, span(c, B)]

    def x_onward():
        xgot[0].wait()
        ref = xo.reshape(R, 2, R, B, B).at[:, :, x]
        for d in (PLUS, MINUS, FAR):
            send(xsend, ref, ref, {"x": at("x", d)}, xgot[1])

    a_wait()
    wsib.wait()
    down(0, 0)
    down(0, 1)
    w_near(0, range(2))
    w_near(1, range(2))
    for lane in range(2):
        w_far(0, lane)
        w_far(1, lane)
    o_send((FAR,), zg2[1])
    w_onward(2)
    w_near(0, (2,))
    early(1, 0)
    w_onward(3)
    early(1, 1)
    add(0, 0)
    w_near(0, (NP - 1,))
    down(1, 0)
    w_near(1, (2, NP - 1))
    down(1, 1)
    add(0, 1)
    early(2, 0)
    down(2, 0)
    early(2, 1)
    down(2, 1)
    add(1, 0)
    add(1, 1)
    og2.wait()
    zg2[0].wait()
    resid(0, 0)
    tell(0, 0)
    resid(0, 1)
    x_out(0)
    q_onward(3)
    q_last(0)
    q_last(2)
    add(2, 0)
    resid(1, 0)
    tell(1, 0)
    add(2, 1)
    far(0)
    resid(1, 1)
    x_out(1)
    wlast[0].wait()
    down_last(0, 0)
    down_last(0, 1)
    resid(2, 0)
    tell(2, 0)
    far(1)
    tell(0, 1)
    wlast[1].wait()
    down_last(1, 0)
    down_last(1, 1)
    resid(2, 1)
    x_out(2)
    zg2[1].wait()
    resid_last(0, 0)
    tell(3, 0, 0)
    resid_last(0, 1)
    q_last(1)
    q_last(3)
    resid_last(1, 0)
    tell(3, 0, 1)
    tell(1, 1)
    tell(2, 1)
    tell(3, 1, 0)
    resid_last(1, 1)
    tell(3, 1, 1)
    x_out(3)
    qsib.wait()

    def qrow(zz, yy, off, n):
        return qo.at[ahead(((zz * 2 + c) * R + yy) * B + off, n, Q), :]

    osend, osib = Sends(qo.at[0:31 * B]), Got(qo.at[0:D // 2])

    def qkv(h):
        t = halves(h)

        @pl.when(x == y)
        def _():
            ngot[h].wait(N2.at[:, 0:H, 0:6 * B])

        @pl.when(x != y)
        def _():
            ngot[h].wait()
        norm(N2, G2F, N2B, h * H, h * H, H)
        for j in range(3):
            cols = slice(j * 3 * B, (j + 1) * 3 * B)
            w = WQ[:, :, :, cols].reshape(D, 3 * B)
            qo[ahead(((z * 2 + c) * R + y) * B + h * H, H, H), cols] = jnp.dot(
                N2B[t, :], w, preferred_element_type=F32).astype(BF)
            fan[h](cols)

    def out_sib(ref):
        send(osend, ref, ref, sib, osib)

    todo = {}

    def coming(name, ref, then, whole):
        todo[name] = (Got(ref), then, whole)

    def arrivals(h):
        first, second = "yz" if h == 0 else "zy"

        def block(i, j, off, n):
            a, b = at(first, i), at(second, j)
            return qrow(b if h == 0 else a, a if h == 0 else b, h * H + off, n)

        def hop(axis, d, ref, name):
            send(osend, ref, ref, {axis: at(axis, d)}, todo[name][0])

        def across(name, i, parts):
            def start():
                for off, n, part in parts:
                    for d in (PLUS, MINUS):
                        hop(second, d, block(i, 0, off, n), f"s{h}{name}{part}{d}")
            for off, n, part in parts:
                for u, d in enumerate((PLUS, MINUS)):
                    def onward(u=u, d=d, off=off, part=part):
                        if part in ("", str(u)):
                            hop(second, d, block(i, R - d, u * Q, Q), f"l{h}{name}{u}")
                    coming(f"s{h}{name}{part}{d}", block(i, R - d, off, n), onward, block(i, R - d, off, n))
            for u in range(2):
                ref = block(i, FAR, u * Q, Q)
                coming(f"l{h}{name}{u}", ref, None, ref)
            return start

        full = [(0, H, "")]
        go = {name: across(name, i, full) for name, i in (("o", 0), ("m", MINUS), ("p", PLUS))}
        across("f", FAR, [(0, Q, "0"), (Q, Q, "1")])
        for u, (d, name) in enumerate(((PLUS, "m"), (MINUS, "p"))):
            def onward(u=u, d=d, name=name):
                hop(first, d, block(R - d, 0, u * Q, Q), f"r{h}{u}")
                go[name]()
            coming(f"f{h}{d}", block(R - d, 0, 0, H), onward, block(R - d, 0, 0, H))
            ref = block(FAR, 0, u * Q, Q)

            def rest(u=u):
                for d in (PLUS, MINUS):
                    hop(second, d, block(FAR, 0, u * Q, Q), f"s{h}f{u}{d}")
            coming(f"r{h}{u}", ref, rest, ref)

        def own(cols):
            ref = block(0, 0, 0, H).at[:, cols]
            for d in (PLUS, MINUS):
                hop(first, d, ref, f"f{h}{d}")
            for d in (PLUS, MINUS):
                hop(second, d, ref, f"s{h}o{d}")
            out_sib(ref)
        return own

    fan = [arrivals(h) for h in range(2)]
    for h in range(2):
        qkv(h)
    x_onward()
    for key in ("f0", "s0o", "s1o", "f1", "r0", "s0m", "l1o", "s0p", "s1m", "l0o", "r1", "s1p",
                "s0f0", "l1m", "s0f1", "s1f0", "l0m", "s1f1", "l0p", "l1p", "l0f", "l1f"):
        for name in [n for n in todo if n.startswith(key)]:
            got, then, ref = todo.pop(name)
            got.wait()
            if then:
                then()
            out_sib(ref)
    assert not todo
    osib.wait()
    xgot[1].wait()
    for s in sends:
        s.wait()

    @pl.when(x == y)
    def _():
        r = N2.at[:, :, 0:6 * B]
        pltpu.make_async_copy(r, r, ss.at[nsend]).wait()

    @pl.when(x != y)
    def _():
        pltpu.make_async_copy(N2, N2, ss.at[nsend]).wait()


def _copy(a, b, c, d, sem):
    n = 4
    cps = []
    for i, (src, dst) in enumerate(((a, c), (b, d))):
        for j in range(n):
            r = slice(j * D // n, (j + 1) * D // n)
            cps.append(pltpu.make_async_copy(src.at[r], dst.at[r], sem.at[i, j]))
            cps[-1].start()
    for cp in cps:
        cp.wait()


def solution(mesh):
    mesh4 = Mesh(mesh.devices.reshape(R, R, R, 2), ("x", "z", "y", "c"))

    def body(x, g1, g2, w_gate, w_up, w_down, o, w_o, w_qkv):
        vm = pltpu.VMEM
        anyspec = pl.BlockSpec(memory_space=pl.ANY)
        sem = pltpu.SemaphoreType.DMA
        outs = pl.pallas_call(
            _kernel,
            out_shape=(vm((D, B), BF), vm((D, W), BF)),
            in_specs=[anyspec] * 9,
            out_specs=(pl.BlockSpec(memory_space=vm), pl.BlockSpec(memory_space=vm)),
            scratch_shapes=[
                vm((R, 2, B, B), BF),
                vm((R, B, DZ), BF),
                vm((R, 1, B), F32), vm((R, 1, B), F32),
                vm((R, 1, DZ), F32), vm((R, 1, DZ), F32),
                vm((DZ, D), BF),
                vm((NQ, D, 2 * B), BF),
                vm((NQ, 2, R, B, B), BF),
                vm((R, B, D), BF),
                vm((R, 2 * B, DZ), BF),
                vm((DZ, B), BF),
                vm((R - 1, R, 2, B, B), F32),
                vm((R, 2, B, B), F32),
                vm((R, B, 2 * B), F32),
                vm((R, D, 2 * B), BF),
                vm((R, 2, R, B, B), F32),
                vm((R, R - 1, 2, B, B), F32),
                vm((R, B, 2 * B), BF),
                vm((R, B, DZ), BF),
                vm((B, D), BF),
                vm((R, 8, B, W), BF),
                sem((NSEND,)), sem((NRECV,)), sem((NLOC,)),
            ],
            compiler_params=pltpu.CompilerParams(
                collective_id=0, has_side_effects=True, vmem_limit_bytes=53 * 2**20),
            name="block",
        )(x.reshape(R, 2, R, B, B), g1.reshape(1, B), g2.reshape(1, B), w_gate, w_up, w_down, o, w_o, w_qkv)
        return pl.pallas_call(
            _copy,
            out_shape=(jax.ShapeDtypeStruct((D, B), BF), jax.ShapeDtypeStruct((D, W), BF)),
            in_specs=[pl.BlockSpec(memory_space=vm)] * 2,
            out_specs=(anyspec, anyspec),
            scratch_shapes=[sem((2, 4))],
            compiler_params=pltpu.CompilerParams(vmem_limit_bytes=2**20),
            name="store",
        )(*outs)

    h = ("z", "y", "c")
    in_specs = (P(None, h), P(h), P(h), P(h, "x"), P(h, "x"), P("x", h), P(None, "x"), P("x", h), P(h, "x"))
    return jax.shard_map(body, mesh=mesh4, in_specs=in_specs, out_specs=(P(None, h), P(None, "x")), check_vma=False)
```

```python
import jax
import jax.numpy as jnp
from jax import lax
from jax.experimental import pallas as pl
from jax.experimental.pallas import tpu as pltpu
from jax.sharding import Mesh, PartitionSpec as P

EPS = 1e-6
MESH = pl.DeviceIdType.MESH
BF = jnp.bfloat16
F32 = jnp.float32
R = 4
B = 128
H = B // 2
Q = H // 2
D = 4096
DZ = D // R
DC = DZ // 2
NQ = 4
NP = 4
W = 1152
NSEND, NRECV, NLOC = 21, 156, 19


def _kernel(x5, g1, g2, wg, wu, wd, o, wo, wq, xo, qo,
            XR, XN, G1S, G2S, G1F, G2F, NF, WGU, AL, AF, OT, WO, OR, OS, OD, WD, PB, RB, XP, N2, N2B, WQ,
            ss, rs, ls):
    x, y, z, c = (lax.axis_index(a) for a in "xyzc")
    here = {"x": x, "y": y, "z": z}

    def at(axis, d):
        return lax.rem(here[axis] + d, R)

    PLUS, MINUS, FAR = 1, R - 1, 2
    oc = 1 - c
    sib = {"c": oc}
    blk = y * 2 + c

    count = {"s": 0, "r": 0, "l": 0}
    limit = {"s": NSEND, "r": NRECV, "l": NLOC}

    def new(kind):
        count[kind] += 1
        assert count[kind] <= limit[kind]
        return count[kind] - 1

    sends = []

    class Sends:
        def __init__(self, ref):
            self.i, self.ref = new("s"), ref
            sends.append(self)

        def wait(self):
            pltpu.make_async_copy(self.ref, self.ref, ss.at[self.i]).wait()

    class Got:
        def __init__(self, ref):
            self.i, self.ref = new("r"), ref

        def wait(self, ref=None):
            ref = self.ref if ref is None else ref
            pltpu.make_async_copy(ref, ref, rs.at[self.i]).wait()

    def send(group, src, dst, dev, got):
        d = pltpu.make_async_remote_copy(
            src_ref=src, dst_ref=dst, send_sem=ss.at[group.i], recv_sem=rs.at[got.i],
            device_id=dev, device_id_type=MESH)
        d.start()

    def here_copy(src, dst, got):
        pltpu.make_async_copy(src, dst, rs.at[got.i]).start()

    def load(src, dst):
        d = pltpu.make_async_copy(src, dst, ls.at[new("l")])
        d.start()
        return d

    def span(b, n):
        return pl.ds(pl.multiple_of(b * n, n), n)

    def ahead(b, n, step):
        return pl.ds(pl.multiple_of(b, step), n)

    bar = pltpu.get_barrier_semaphore()
    peers = [(dx, 0, 0, 0) for dx in range(1, R)]
    peers += [(0, dy, 0, dc) for dy in range(R) for dc in range(2) if dy + dc]
    peers += [(0, 0, dz, dc) for dz in range(1, R) for dc in range(2)]
    for dx, dy, dz, dc in peers:
        pl.semaphore_signal(bar, inc=1, device_id={
            "x": at("x", dx), "y": at("y", dy), "z": at("z", dz), "c": oc if dc else c}, device_id_type=MESH)

    DIST = (0, PLUS, MINUS, FAR)
    l_wo = load(wo, WO)
    NT = D // (2 * B)
    tiles = [pltpu.make_async_copy(o.at[i * 2 * B:(i + 1) * 2 * B, :], OT.at[i % R], ls.at[new("l")]) for i in range(NT)]
    for i in range(R):
        tiles[i].start()
    l_wd = load(wd, WD.at[z, :, span(c, B)])
    l_wq = load(wq, WQ.at[z, blk])
    pl.semaphore_wait(bar, len(peers))

    near = [(dy, dc) for dy in (PLUS, MINUS, FAR, 0) for dc in range(2) if dy + dc]

    def yc(dy, dc):
        return at("y", dy), (oc if dc else c)

    firsts = ((x5, XR, XN), (g1, G1S, G1F), (g2, G2S, G2F))
    s1, s1s = [Got(b) for _, b, _ in firsts], [Sends(b.at[0:R - 1]) for _, b, _ in firsts]
    for dz in (PLUS, MINUS, FAR, 0):
        z2 = at("z", dz)
        for (src, dst, _), got, grp in zip(firsts, s1, s1s):
            s = src.at[z2, :, x] if src is x5 else src
            if dz:
                send(grp, s, dst.at[z], {"z": z2}, got)
            else:
                here_copy(s, dst.at[z], got)

    a2a, a2as = [Got(WGU.at[q, span(z, DZ), :]) for q in range(NQ)], Sends(NF.at[0:NQ * 7 * 8, :])

    def send_a2a(q):
        r = span(z * 8 + blk, B)
        for dy, dc in near + [(0, 0)]:
            y2, c2 = yc(dy, dc)
            cols = span((y2 * 2 + c2) * NQ + q, B)
            for w, off in ((wg, 0), (wu, B)):
                s, d = w.at[:, cols], WGU.at[q, r, off:off + B]
                if dy + dc:
                    send(a2as, s, d, {"y": y2, "c": c2}, a2a[q])
                else:
                    here_copy(s, d, a2a[q])

    class Ring:
        def __init__(self, axis, sends, own, half):
            self.axis, self.sends, self.half = axis, sends, half
            self.got = [Got(own), Got(own)]
            self.far = Got(own)

        def own(self, src, dst):
            for d, g in zip((PLUS, MINUS), self.got):
                send(self.sends, src, dst, {self.axis: at(self.axis, d)}, g)

        def wait(self):
            for g in self.got:
                g.wait()

        def onward(self):
            for h, d in enumerate((PLUS, MINUS)):
                ref = self.half(at(self.axis, R - d), h)
                send(self.sends, ref, ref, {self.axis: at(self.axis, d)}, self.far)

        def wait_far(self):
            self.far.wait()

    send_a2a(0)
    send_a2a(1)
    qz = Ring("z", Sends(WQ.at[0, 0:R - 1]), WQ.at[0, 0], lambda zz, h: WQ.at[zz, blk, h * H:h * H + H])
    qz.own(wq, WQ.at[z, blk])

    wds = Sends(WD.at[:, 0:D * 7 // 8, :])
    cuts = [(p, p * DZ, (p + 1) * DZ) for p in range(NP)]
    wgot = [[Got(WD.at[0, s:e, 0:B]), Got(WD.at[0, s:e, 0:B])] for _, s, e in cuts]
    piece = WD.at[0, 0:DZ, 0:B]
    wsib, wnear = Got(WD.at[0, :, 0:B]), [[Got(piece), Got(piece)] for _ in range(NP)]
    wfar, wlast = [[Got(piece), Got(piece)] for _ in range(2)], [Got(WD.at[0, 0:2 * DZ, 0:B]) for _ in range(2)]

    def cut(i, h):
        p = (i + 2 * h) % NP
        return cuts[p]

    def w_own(i):
        for h, (d, g) in enumerate(zip((PLUS, MINUS), wgot[i])):
            _, s, e = cut(i, h)
            send(wds, wd.at[s:e, :], WD.at[z, s:e, span(c, B)], {"z": at("z", d)}, g)
        _, s, e = cuts[i]
        send(wds, wd.at[s:e, :], WD.at[z, s:e, span(c, B)], sib, wsib)

    def w_onward(i):
        for h, (d, g) in enumerate(zip((PLUS, MINUS), wgot[i])):
            g.wait()
            _, s, e = cut(i, h)
            ref = WD.at[at("z", R - d), s:e, span(c, B)]
            send(wds, ref, ref, sib, wnear[i][h])

    def w_near(h, ps):
        for p in ps:
            wnear[p][h].wait()

    def w_far(h, lane):
        d = (PLUS, MINUS)[h]
        ref = WD.at[at("z", R - d), span(2 * h + c, DZ), lane * B:(lane + 1) * B]
        send(wds, ref, ref, {"z": at("z", d)}, wfar[lane][h])

    def far(lane):
        for h, g in enumerate(wfar[lane]):
            g.wait()
            ref = WD.at[at("z", FAR), span(2 * h + c, DZ), lane * B:(lane + 1) * B]
            send(wds, ref, ref, sib, wlast[lane])

    l_wo.wait()
    os, og = Sends(OR), Got(OR)
    for i in range(NT):
        tiles[i].wait()
        p, q, r = i // 2 // 2, i // 2 % 2, i % 2 * 2
        PB[p, q, r:r + 2] = jnp.dot(OT[i % R], WO[...], preferred_element_type=F32).reshape(2, B, B)
        if i + R < NT:
            tiles[i + R].start()
        if q and r:
            for j, d in enumerate((PLUS, MINUS, FAR)):
                send(os, PB.at[p, :, at("x", d)], OR.at[j, p], {"x": at("x", d)}, og)
    for g in s1:
        g.wait()
    less = slice(0, 7 * B)
    s2, s2s = [Got(b.at[:, :, less]) for _, _, b in firsts], [Sends(b.at[:, :, less]) for _, _, b in firsts]
    for dy, dc in near:
        y2, c2 = yc(dy, dc)
        for (_, src, dst), got, grp in zip(firsts, s2, s2s):
            send(grp, src.at[:, c2] if src is XR else src, dst.at[:, :, span(blk, B)], {"y": y2, "c": c2}, got)
    for q in range(2, NQ):
        send_a2a(q)
    XN[:, :, span(blk, B)] = XR[:, c]
    G1F[:, :, span(blk, B)] = G1S[...]
    G2F[:, :, span(blk, B)] = G2S[...]

    zs = Sends(NF.at[0:NQ * R * (R - 1) * 16, :])
    zr = [Ring("z", zs, WGU.at[q, 0:DZ, :],
               lambda zz, h, q=q: WGU.at[q, span(zz * 2 + h, DC), :]) for q in range(NQ)]

    def z_own(q):
        a2a[q].wait()
        ref = WGU.at[q, span(z, DZ), :]
        zr[q].own(ref, ref)

    def z_onward(q):
        zr[q].wait()
        zr[q].onward()

    z_own(0)
    z_own(1)
    qz.wait()
    qz.onward()

    def norm(src, gain, dst, base, first, n):
        def step(i, _):
            r = span(first // 16 + i, 16)
            v = [src[k, r, :].astype(F32) for k in range(R)]
            s = sum(jnp.sum(t * t, axis=-1, keepdims=True) for t in v)
            inv = lax.rsqrt(s / D + EPS)
            for k in range(R):
                dst[ahead(base + i * 16, 16, 16), k * DZ:(k + 1) * DZ] = (v[k] * inv * gain[k]).astype(BF)
            return 0
        lax.fori_loop(0, n // 16, step, 0)

    for g in s2:
        g.wait()
    nrow = c * R + x
    norm(XN, G1F, NF, nrow * B, 0, B)

    def nhalf(xx, h):
        return NF.at[span((c * R + xx) * 2 + h, H), :]

    ns, nsib = Sends(NF.at[0:7 * B, :]), [Got(NF.at[0:3 * B, :]), Got(NF.at[0:B, :])]
    xr = Ring("x", ns, NF.at[0:B, :], nhalf)

    def n_sib(xx, got):
        ref = NF.at[span(c * R + xx, B), :]
        send(ns, ref, ref, sib, got)

    ref = NF.at[span(nrow, B), :]
    xr.own(ref, ref)
    n_sib(x, nsib[0])
    z_onward(0)
    z_own(2)
    qz.wait_far()
    l_wq.wait()
    qys, qsib = Sends(WQ.at[:, 0:7]), Got(WQ.at[:, 0:R])
    slab = WQ.at[0, 0]
    qgot = [[Got(slab), Got(slab)] for _ in range(R)]
    qfar = [Got(slab) for _ in range(R)]

    def q_own(j):
        ref = WQ.at[j, blk]
        for d, g in zip((PLUS, MINUS), qgot[j]):
            send(qys, ref, ref, {"y": at("y", d)}, g)
        send(qys, ref, ref, sib, qsib)

    def q_onward(j):
        for i, (d, g) in enumerate(zip((PLUS, MINUS), qgot[j])):
            g.wait()
            ref = WQ.at[j, at("y", R - d) * 2 + c]
            if i == j // 2:
                send(qys, ref, ref, {"y": at("y", d)}, qfar[j])
            send(qys, ref, ref, sib, qsib)

    def q_last(j):
        qfar[j].wait()
        ref = WQ.at[j, at("y", FAR) * 2 + c]
        send(qys, ref, ref, sib, qsib)

    for j in (0, 2, 1):
        q_own(j)
    z_onward(1)
    z_own(3)
    xr.wait()
    xr.onward()
    n_sib(at("x", MINUS), nsib[0])
    n_sib(at("x", PLUS), nsib[0])

    og.wait()
    OS[...] = PB[:, :, x] + OR[0] + OR[1] + OR[2]
    zs2, zg2 = Sends(OD.at[0:R - 1]), [Got(OD.at[0:2]), Got(OD.at[0])]
    os2, og2 = Sends(OD.at[0, :, 0:B]), Got(OD.at[0, :, 0:B])
    os.wait()
    sends.remove(os)

    def o_send(ds, got):
        for d in ds:
            for c2 in (c, oc):
                send(zs2, OS.at[at("z", d), c2], OD.at[z, :, span(c, B)], {"z": at("z", d), "c": c2}, got)

    units = [[(0, 0, 3)], [(1, 0, 3)], [(0, 3, R), (1, 3, R)], [(2, 0, 2)], [(2, 2, R)], [(3, 0, 2)], [(3, 2, R)]]
    asend = Sends(AF.at[:, :, 0:NQ * 7 * B])
    arest = Got(AF.at[:, :, 0:NQ * 5 * B])
    agot = []
    for u in units:
        n = AF.at[0:sum(hi - lo for _, lo, hi in u), :, 0:B]
        agot.append([Got(n), Got(n)])
    NF4 = NF.reshape(2, R, B, D)

    def act(u):
        for q, lo, hi in units[u]:
            def step(s, _):
                xb = at("x", s + s // 2 - s // 3 * 2)
                gu = jnp.dot(NF4[:, xb].reshape(2 * B, D), WGU[q], preferred_element_type=F32)
                g, up = gu[:, :B], gu[:, B:]
                AL[q, :, s] = (g * lax.logistic(g) * up).astype(BF).reshape(2, B, B)
                return 0
            lax.fori_loop(lo, hi, step, 0)
            col = span(blk * NQ + q, B)
            dst = AF.at[lo:hi, :, col]
            for i, d in enumerate((PLUS, MINUS)):
                for c2 in range(2):
                    for c1 in range(2):
                        @pl.when(c == c1)
                        def _():
                            send(asend, AL.at[q, c2, lo:hi], dst, {"y": at("y", d), "c": c2}, agot[u][i] if c1 == i else arest)
            send(asend, AL.at[q, oc, lo:hi], dst, sib, arest)
            AF[lo:hi, :, col] = AL[q, c, lo:hi]

    def a_onward(u):
        for i, d in enumerate((PLUS, MINUS)):
            agot[u][i].wait()
            for q, lo, hi in units[u]:
                ref = AF.at[lo:hi, :, span((at("y", R - d) * 2 + i) * NQ + q, B)]
                send(asend, ref, ref, {"y": at("y", d)}, arest)

    nsib[0].wait()
    zr[0].wait_far()
    act(0)
    z_onward(2)
    zr[1].wait_far()
    act(1)
    xr.wait_far()
    n_sib(at("x", FAR), nsib[1])
    a_onward(0)
    nsib[1].wait()
    act(2)
    a_onward(1)
    z_onward(3)
    q_onward(0)
    q_onward(2)
    for p in range(NP):
        w_own(p)
    send(os2, OS.at[z, oc], OD.at[z, :, span(c, B)], sib, og2)
    OD[z, :, span(c, B)] = OS[z, c]
    a_onward(2)
    zr[2].wait_far()
    act(3)
    act(4)
    zr[3].wait_far()
    act(5)
    act(6)
    a_onward(3)
    a_onward(4)
    w_onward(0)
    a_onward(5)
    a_onward(6)
    q_own(3)
    q_onward(1)
    w_onward(1)
    l_wd.wait()

    zk = [z, at("z", MINUS), at("z", PLUS), at("z", FAR)]
    rsend = [Sends(RB.at[0:R - 1]), Sends(RB.at[0])]
    block = RB.at[0, 0, 0, 0:H]
    rgot = [[[Got(block), Got(block), Got(RB.at[k, 0:2, :, 0:H])] for _ in range(2)] for k in range(R - 1)]
    rlast = [[Got(RB.at[0, :, 0, 0:H]) for _ in range(2)] for _ in range(2)]
    ngot = [Got(N2.at[:, 0:H]) for _ in range(2)]
    xgot, xsend = [Got(xo.at[0:7 * B]), Got(xo.at[0:24 * B])], Sends(xo.at[0:31 * B])
    nsend = new("s")

    def halves(h):
        return slice(h * H, h * H + H)

    def product(k, h, w, kk=slice(0, D)):
        return jnp.dot(AF[:, halves(h), kk].reshape(2 * B, w.shape[0]), w, preferred_element_type=F32)

    def early(k, h):
        spans = [slice(0, D - DZ)] if k == 1 else [slice(2 * DZ, D), slice(0, DZ)]
        p = sum(product(k, h, WD[zk[k], kk], kk) for kk in spans)
        for i in range(2):
            PB[k, i, :, halves(h)] = p[:, i * B:(i + 1) * B].reshape(R, H, B)

    def down_last(i, h):
        t, k = halves(h), R - 1
        p = product(k, h, WD[zk[k], :, i * B:(i + 1) * B])
        PB[k, i, :, t] = p.reshape(R, H, B)
        for j, d in enumerate(DIST):
            if j:
                send(rsend[1], PB.at[k, i, j, t], RB.at[k, j - 1, i, t], {"x": at("x", d)}, rlast[i][h])

    def down(k, h):
        t = halves(h)
        kk = (slice(0, D), slice(D - DZ, D), slice(DZ, 2 * DZ))[k]
        p = product(k, h, WD[zk[k], kk], kk)
        for i in range(2):
            v = p[:, i * B:(i + 1) * B].reshape(R, H, B)
            PB[k, i, :, t] = PB[k, i, :, t] + v if k else v
        for i, d in enumerate((PLUS, MINUS)):
            to = {"x": at("x", d)}
            send(rsend[0], PB.at[k, i, R - 1, t], RB.at[k, R - 2, i, t], to, rgot[k][h][i])
            send(rsend[0], PB.at[k, 1 - i, 1 + i, t], RB.at[k, i, 1 - i, t], to, rgot[k][h][2])

    def add(k, h):
        t = halves(h)
        for i, d in enumerate((PLUS, MINUS)):
            rgot[k][h][i].wait()
            PB[k, i, 1 + i, t] = PB[k, i, 1 + i, t] + RB[k, R - 2, i, t]
            send(rsend[0], PB.at[k, i, 1 + i, t], RB.at[k, i, i, t], {"x": at("x", d)}, rgot[k][h][2])

    def finish(k, h, i, yy):
        t, part = halves(h), slice(i * B, (i + 1) * B)
        XP[k, t, part] = (XN[zk[k], t, span(y * 2 + i, B)].astype(F32) + (OD[zk[k], t, part] + PB[k, i, 0, t] + yy)).astype(BF)

    def resid(k, h):
        t = halves(h)
        rgot[k][h][2].wait()
        for i in range(2):
            finish(k, h, i, RB[k, 0, i, t] + RB[k, 1, i, t])

    def resid_last(i, h):
        t, k = halves(h), R - 1
        rlast[i][h].wait()
        finish(k, h, i, RB[k, 0, i, t] + RB[k, 1, i, t] + RB[k, 2, i, t])

    def tell(k, h, i=None):
        t = halves(h)
        if i is None:
            src, dst = XP.at[k, t], N2.at[zk[k], t, span(y, 2 * B)]
        else:
            src, dst = XP.at[k, t, i * B:(i + 1) * B], N2.at[zk[k], t, span(y * 2 + i, B)]
        for d in range(R):
            cp = pltpu.make_async_remote_copy(
                src_ref=src, dst_ref=dst, send_sem=ss.at[nsend], recv_sem=rs.at[ngot[h].i],
                device_id={"x": at("x", d), "y": x}, device_id_type=MESH)
            if d:
                cp.start()
            else:
                pl.when(x != y)(cp.start)

                @pl.when(x == y)
                def _():
                    dst[...] = src[...]

    def x_out(k):
        rows = xo.at[span((z * 2 + c) * R + x, B), :]
        send(xsend, XP.at[k, :, span(oc, B)], rows, {"z": zk[k], "c": oc}, xgot[0])
        if k:
            send(xsend, XP.at[k, :, span(c, B)], rows, {"z": zk[k]}, xgot[0])
        else:
            rows[...] = XP[k, :, span(c, B)]

    def x_onward():
        xgot[0].wait()
        ref = xo.reshape(R, 2, R, B, B).at[:, :, x]
        for d in (PLUS, MINUS, FAR):
            send(xsend, ref, ref, {"x": at("x", d)}, xgot[1])

    arest.wait()
    wsib.wait()
    down(0, 0)
    down(0, 1)
    w_near(0, range(2))
    w_near(1, range(2))
    for lane in range(2):
        w_far(0, lane)
        w_far(1, lane)
    o_send((PLUS, MINUS), zg2[0])
    o_send((FAR,), zg2[1])
    w_onward(2)
    w_near(0, (2,))
    early(1, 0)
    w_onward(3)
    early(1, 1)
    add(0, 0)
    w_near(0, (NP - 1,))
    down(1, 0)
    w_near(1, (2, NP - 1))
    down(1, 1)
    add(0, 1)
    early(2, 0)
    down(2, 0)
    early(2, 1)
    down(2, 1)
    add(1, 0)
    add(1, 1)
    og2.wait()
    resid(0, 0)
    tell(0, 0)
    resid(0, 1)
    x_out(0)
    q_onward(3)
    q_last(0)
    q_last(2)
    add(2, 0)
    add(2, 1)
    far(0)
    wlast[0].wait()
    down_last(0, 0)
    down_last(0, 1)
    tell(0, 1)
    far(1)
    wlast[1].wait()
    down_last(1, 0)
    down_last(1, 1)
    zg2[0].wait()
    for k in (1, 2):
        resid(k, 0)
        tell(k, 0)
    for k in (1, 2):
        resid(k, 1)
        x_out(k)
    zg2[1].wait()
    resid_last(0, 0)
    tell(3, 0, 0)
    resid_last(0, 1)
    q_last(1)
    q_last(3)
    resid_last(1, 0)
    tell(3, 0, 1)
    tell(1, 1)
    tell(2, 1)
    tell(3, 1, 0)
    resid_last(1, 1)
    tell(3, 1, 1)
    x_out(3)
    qsib.wait()

    def qrow(zz, yy, off, n):
        return qo.at[ahead(((zz * 2 + c) * R + yy) * B + off, n, Q), :]

    osend, osib = Sends(qo.at[0:31 * B]), Got(qo.at[0:D // 2])

    def qkv(h):
        t = halves(h)

        @pl.when(x == y)
        def _():
            ngot[h].wait(N2.at[:, 0:H, 0:6 * B])

        @pl.when(x != y)
        def _():
            ngot[h].wait()
        norm(N2, G2F, N2B, h * H, h * H, H)
        for j in range(3):
            cols = slice(j * 3 * B, (j + 1) * 3 * B)
            w = WQ[:, :, :, cols].reshape(D, 3 * B)
            qo[ahead(((z * 2 + c) * R + y) * B + h * H, H, H), cols] = jnp.dot(
                N2B[t, :], w, preferred_element_type=F32).astype(BF)
            fan[h](cols)

    def out_sib(ref):
        send(osend, ref, ref, sib, osib)

    todo = {}

    def coming(name, ref, then, whole):
        todo[name] = (Got(ref), then, whole)

    def arrivals(h):
        first, second = "yz" if h == 0 else "zy"

        def block(i, j, off, n):
            a, b = at(first, i), at(second, j)
            return qrow(b if h == 0 else a, a if h == 0 else b, h * H + off, n)

        def hop(axis, d, ref, name):
            send(osend, ref, ref, {axis: at(axis, d)}, todo[name][0])

        def across(name, i, parts):
            def start():
                for off, n, part in parts:
                    for d in (PLUS, MINUS):
                        hop(second, d, block(i, 0, off, n), f"s{h}{name}{part}{d}")
            for off, n, part in parts:
                for u, d in enumerate((PLUS, MINUS)):
                    def onward(u=u, d=d, off=off, part=part):
                        if part in ("", str(u)):
                            hop(second, d, block(i, R - d, u * Q, Q), f"l{h}{name}{u}")
                    coming(f"s{h}{name}{part}{d}", block(i, R - d, off, n), onward, block(i, R - d, off, n))
            for u in range(2):
                ref = block(i, FAR, u * Q, Q)
                coming(f"l{h}{name}{u}", ref, None, ref)
            return start

        full = [(0, H, "")]
        go = {name: across(name, i, full) for name, i in (("o", 0), ("m", MINUS), ("p", PLUS))}
        across("f", FAR, [(0, Q, "0"), (Q, Q, "1")])
        for u, (d, name) in enumerate(((PLUS, "m"), (MINUS, "p"))):
            def onward(u=u, d=d, name=name):
                hop(first, d, block(R - d, 0, u * Q, Q), f"r{h}{u}")
                go[name]()
            coming(f"f{h}{d}", block(R - d, 0, 0, H), onward, block(R - d, 0, 0, H))
            ref = block(FAR, 0, u * Q, Q)

            def rest(u=u):
                for d in (PLUS, MINUS):
                    hop(second, d, block(FAR, 0, u * Q, Q), f"s{h}f{u}{d}")
            coming(f"r{h}{u}", ref, rest, ref)

        def own(cols):
            ref = block(0, 0, 0, H).at[:, cols]
            for d in (PLUS, MINUS):
                hop(first, d, ref, f"f{h}{d}")
            for d in (PLUS, MINUS):
                hop(second, d, ref, f"s{h}o{d}")
            out_sib(ref)
        return own

    fan = [arrivals(h) for h in range(2)]
    for h in range(2):
        qkv(h)
    x_onward()
    for key in ("f0", "s0o", "s1o", "f1", "r0", "s0m", "l1o", "s0p", "s1m", "l0o", "r1", "s1p",
                "s0f0", "l1m", "s0f1", "s1f0", "l0m", "s1f1", "l0p", "l1p", "l0f", "l1f"):
        for name in [n for n in todo if n.startswith(key)]:
            got, then, ref = todo.pop(name)
            got.wait()
            if then:
                then()
            out_sib(ref)
    assert not todo
    osib.wait()
    xgot[1].wait()
    for s in sends:
        s.wait()

    @pl.when(x == y)
    def _():
        r = N2.at[:, :, 0:6 * B]
        pltpu.make_async_copy(r, r, ss.at[nsend]).wait()

    @pl.when(x != y)
    def _():
        pltpu.make_async_copy(N2, N2, ss.at[nsend]).wait()


def _copy(a, b, c, d, sem):
    n = 4
    cps = []
    for i, (src, dst) in enumerate(((a, c), (b, d))):
        for j in range(n):
            r = slice(j * D // n, (j + 1) * D // n)
            cps.append(pltpu.make_async_copy(src.at[r], dst.at[r], sem.at[i, j]))
            cps[-1].start()
    for cp in cps:
        cp.wait()


def solution(mesh):
    mesh4 = Mesh(mesh.devices.reshape(R, R, R, 2), ("x", "z", "y", "c"))

    def body(x, g1, g2, w_gate, w_up, w_down, o, w_o, w_qkv):
        vm = pltpu.VMEM
        anyspec = pl.BlockSpec(memory_space=pl.ANY)
        sem = pltpu.SemaphoreType.DMA
        outs = pl.pallas_call(
            _kernel,
            out_shape=(vm((D, B), BF), vm((D, W), BF)),
            in_specs=[anyspec] * 9,
            out_specs=(pl.BlockSpec(memory_space=vm), pl.BlockSpec(memory_space=vm)),
            scratch_shapes=[
                vm((R, 2, B, B), BF),
                vm((R, B, DZ), BF),
                vm((R, 1, B), F32), vm((R, 1, B), F32),
                vm((R, 1, DZ), F32), vm((R, 1, DZ), F32),
                vm((DZ, D), BF),
                vm((NQ, D, 2 * B), BF),
                vm((NQ, 2, R, B, B), BF),
                vm((R, B, D), BF),
                vm((R, 2 * B, DZ), BF),
                vm((DZ, B), BF),
                vm((R - 1, R, 2, B, B), F32),
                vm((R, 2, B, B), F32),
                vm((R, B, 2 * B), F32),
                vm((R, D, 2 * B), BF),
                vm((R, 2, R, B, B), F32),
                vm((R, R - 1, 2, B, B), F32),
                vm((R, B, 2 * B), BF),
                vm((R, B, DZ), BF),
                vm((B, D), BF),
                vm((R, 8, B, W), BF),
                sem((NSEND,)), sem((NRECV,)), sem((NLOC,)),
            ],
            compiler_params=pltpu.CompilerParams(
                collective_id=0, has_side_effects=True, vmem_limit_bytes=53 * 2**20),
            name="block",
        )(x.reshape(R, 2, R, B, B), g1.reshape(1, B), g2.reshape(1, B), w_gate, w_up, w_down, o, w_o, w_qkv)
        return pl.pallas_call(
            _copy,
            out_shape=(jax.ShapeDtypeStruct((D, B), BF), jax.ShapeDtypeStruct((D, W), BF)),
            in_specs=[pl.BlockSpec(memory_space=vm)] * 2,
            out_specs=(anyspec, anyspec),
            scratch_shapes=[sem((2, 4))],
            compiler_params=pltpu.CompilerParams(vmem_limit_bytes=2**20),
            name="store",
        )(*outs)

    h = ("z", "y", "c")
    in_specs = (P(None, h), P(h), P(h), P(h, "x"), P(h, "x"), P("x", h), P(None, "x"), P("x", h), P(h, "x"))
    return jax.shard_map(body, mesh=mesh4, in_specs=in_specs, out_specs=(P(None, h), P(None, "x")), check_vma=False)
```

```python
import jax
import jax.numpy as jnp
from jax import lax
from jax.experimental import pallas as pl
from jax.experimental.pallas import tpu as pltpu
from jax.sharding import Mesh, PartitionSpec as P

EPS = 1e-6
MESH = pl.DeviceIdType.MESH
BF = jnp.bfloat16
F32 = jnp.float32
R = 4
B = 128
H = B // 2
Q = H // 2
D = 4096
DZ = D // R
DC = DZ // 2
NQ = 4
NP = 4
W = 1152
NSEND, NRECV, NLOC = 21, 156, 19


def _kernel(x5, g1, g2, wg, wu, wd, o, wo, wq, xo, qo,
            XR, XN, G1S, G2S, G1F, G2F, NF, WGU, AL, AF, OT, WO, OR, OS, OD, WD, PB, RB, XP, N2, N2B, WQ,
            ss, rs, ls):
    x, y, z, c = (lax.axis_index(a) for a in "xyzc")
    here = {"x": x, "y": y, "z": z}

    def at(axis, d):
        return lax.rem(here[axis] + d, R)

    PLUS, MINUS, FAR = 1, R - 1, 2
    oc = 1 - c
    sib = {"c": oc}
    blk = y * 2 + c

    count = {"s": 0, "r": 0, "l": 0}
    limit = {"s": NSEND, "r": NRECV, "l": NLOC}

    def new(kind):
        count[kind] += 1
        assert count[kind] <= limit[kind]
        return count[kind] - 1

    sends = []

    class Sends:
        def __init__(self, ref):
            self.i, self.ref = new("s"), ref
            sends.append(self)

        def wait(self):
            pltpu.make_async_copy(self.ref, self.ref, ss.at[self.i]).wait()

    class Got:
        def __init__(self, ref):
            self.i, self.ref = new("r"), ref

        def wait(self, ref=None):
            ref = self.ref if ref is None else ref
            pltpu.make_async_copy(ref, ref, rs.at[self.i]).wait()

    def send(group, src, dst, dev, got):
        d = pltpu.make_async_remote_copy(
            src_ref=src, dst_ref=dst, send_sem=ss.at[group.i], recv_sem=rs.at[got.i],
            device_id=dev, device_id_type=MESH)
        d.start()

    def here_copy(src, dst, got):
        pltpu.make_async_copy(src, dst, rs.at[got.i]).start()

    def load(src, dst):
        d = pltpu.make_async_copy(src, dst, ls.at[new("l")])
        d.start()
        return d

    def span(b, n):
        return pl.ds(pl.multiple_of(b * n, n), n)

    def ahead(b, n, step):
        return pl.ds(pl.multiple_of(b, step), n)

    bar = pltpu.get_barrier_semaphore()
    peers = [(dx, 0, 0, 0) for dx in range(1, R)]
    peers += [(0, dy, 0, dc) for dy in range(R) for dc in range(2) if dy + dc]
    peers += [(0, 0, dz, dc) for dz in range(1, R) for dc in range(2)]
    for dx, dy, dz, dc in peers:
        pl.semaphore_signal(bar, inc=1, device_id={
            "x": at("x", dx), "y": at("y", dy), "z": at("z", dz), "c": oc if dc else c}, device_id_type=MESH)

    DIST = (0, PLUS, MINUS, FAR)
    l_wo = load(wo, WO)
    NT = D // (2 * B)
    tiles = [pltpu.make_async_copy(o.at[i * 2 * B:(i + 1) * 2 * B, :], OT.at[i % R], ls.at[new("l")]) for i in range(NT)]
    for i in range(R):
        tiles[i].start()
    l_wd = load(wd, WD.at[z, :, span(c, B)])
    l_wq = load(wq, WQ.at[z, blk])
    pl.semaphore_wait(bar, len(peers))

    near = [(dy, dc) for dy in (PLUS, MINUS, FAR, 0) for dc in range(2) if dy + dc]

    def yc(dy, dc):
        return at("y", dy), (oc if dc else c)

    firsts = ((x5, XR, XN), (g1, G1S, G1F), (g2, G2S, G2F))
    s1, s1s = [Got(b) for _, b, _ in firsts], [Sends(b.at[0:R - 1]) for _, b, _ in firsts]
    for dz in (PLUS, MINUS, FAR, 0):
        z2 = at("z", dz)
        for (src, dst, _), got, grp in zip(firsts, s1, s1s):
            s = src.at[z2, :, x] if src is x5 else src
            if dz:
                send(grp, s, dst.at[z], {"z": z2}, got)
            else:
                here_copy(s, dst.at[z], got)

    a2a, a2as = [Got(WGU.at[q, span(z, DZ), :]) for q in range(NQ)], Sends(NF.at[0:NQ * 7 * 8, :])

    def send_a2a(q):
        r = span(z * 8 + blk, B)
        for dy, dc in near + [(0, 0)]:
            y2, c2 = yc(dy, dc)
            cols = span((y2 * 2 + c2) * NQ + q, B)
            for w, off in ((wg, 0), (wu, B)):
                s, d = w.at[:, cols], WGU.at[q, r, off:off + B]
                if dy + dc:
                    send(a2as, s, d, {"y": y2, "c": c2}, a2a[q])
                else:
                    here_copy(s, d, a2a[q])

    class Ring:
        def __init__(self, axis, sends, own, half):
            self.axis, self.sends, self.half = axis, sends, half
            self.got = [Got(own), Got(own)]
            self.far = Got(own)

        def own(self, src, dst):
            for d, g in zip((PLUS, MINUS), self.got):
                send(self.sends, src, dst, {self.axis: at(self.axis, d)}, g)

        def wait(self):
            for g in self.got:
                g.wait()

        def onward(self):
            for h, d in enumerate((PLUS, MINUS)):
                ref = self.half(at(self.axis, R - d), h)
                send(self.sends, ref, ref, {self.axis: at(self.axis, d)}, self.far)

        def wait_far(self):
            self.far.wait()

    send_a2a(0)
    send_a2a(1)
    qz = Ring("z", Sends(WQ.at[0, 0:R - 1]), WQ.at[0, 0], lambda zz, h: WQ.at[zz, blk, h * H:h * H + H])
    qz.own(wq, WQ.at[z, blk])

    wds = Sends(WD.at[:, 0:D * 7 // 8, :])
    cuts = [(p, p * DZ, (p + 1) * DZ) for p in range(NP)]
    wgot = [[Got(WD.at[0, s:e, 0:B]), Got(WD.at[0, s:e, 0:B])] for _, s, e in cuts]
    piece = WD.at[0, 0:DZ, 0:B]
    wsib, wnear = Got(WD.at[0, :, 0:B]), [[Got(piece), Got(piece)] for _ in range(NP)]
    wfar, wlast = [[Got(piece), Got(piece)] for _ in range(2)], [Got(WD.at[0, 0:2 * DZ, 0:B]) for _ in range(2)]

    def cut(i, h):
        p = (i + 2 * h) % NP
        return cuts[p]

    def w_own(i):
        for h, (d, g) in enumerate(zip((PLUS, MINUS), wgot[i])):
            _, s, e = cut(i, h)
            send(wds, wd.at[s:e, :], WD.at[z, s:e, span(c, B)], {"z": at("z", d)}, g)
        _, s, e = cuts[i]
        send(wds, wd.at[s:e, :], WD.at[z, s:e, span(c, B)], sib, wsib)

    def w_onward(i):
        for h, (d, g) in enumerate(zip((PLUS, MINUS), wgot[i])):
            g.wait()
            _, s, e = cut(i, h)
            ref = WD.at[at("z", R - d), s:e, span(c, B)]
            send(wds, ref, ref, sib, wnear[i][h])

    def w_near(h, ps):
        for p in ps:
            wnear[p][h].wait()

    def w_far(h, lane):
        d = (PLUS, MINUS)[h]
        ref = WD.at[at("z", R - d), span(2 * h + c, DZ), lane * B:(lane + 1) * B]
        send(wds, ref, ref, {"z": at("z", d)}, wfar[lane][h])

    def far(lane):
        for h, g in enumerate(wfar[lane]):
            g.wait()
            ref = WD.at[at("z", FAR), span(2 * h + c, DZ), lane * B:(lane + 1) * B]
            send(wds, ref, ref, sib, wlast[lane])

    l_wo.wait()
    os, og = Sends(OR), Got(OR)
    for i in range(NT):
        tiles[i].wait()
        p, q, r = i // 2 // 2, i // 2 % 2, i % 2 * 2
        PB[p, q, r:r + 2] = jnp.dot(OT[i % R], WO[...], preferred_element_type=F32).reshape(2, B, B)
        if i + R < NT:
            tiles[i + R].start()
        if q and r:
            for j, d in enumerate((PLUS, MINUS, FAR)):
                send(os, PB.at[p, :, at("x", d)], OR.at[j, p], {"x": at("x", d)}, og)
    for g in s1:
        g.wait()
    less = slice(0, 7 * B)
    s2, s2s = [Got(b.at[:, :, less]) for _, _, b in firsts], [Sends(b.at[:, :, less]) for _, _, b in firsts]
    for dy, dc in near:
        y2, c2 = yc(dy, dc)
        for (_, src, dst), got, grp in zip(firsts, s2, s2s):
            send(grp, src.at[:, c2] if src is XR else src, dst.at[:, :, span(blk, B)], {"y": y2, "c": c2}, got)
    for q in range(2, NQ):
        send_a2a(q)
    XN[:, :, span(blk, B)] = XR[:, c]
    G1F[:, :, span(blk, B)] = G1S[...]
    G2F[:, :, span(blk, B)] = G2S[...]

    zs = Sends(NF.at[0:NQ * R * (R - 1) * 16, :])
    zr = [Ring("z", zs, WGU.at[q, 0:DZ, :],
               lambda zz, h, q=q: WGU.at[q, span(zz * 2 + h, DC), :]) for q in range(NQ)]

    def z_own(q):
        a2a[q].wait()
        ref = WGU.at[q, span(z, DZ), :]
        zr[q].own(ref, ref)

    def z_onward(q):
        zr[q].wait()
        zr[q].onward()

    z_own(0)
    z_own(1)
    qz.wait()
    qz.onward()

    def norm(src, gain, dst, base, first, n):
        def step(i, _):
            r = span(first // 16 + i, 16)
            v = [src[k, r, :].astype(F32) for k in range(R)]
            s = sum(jnp.sum(t * t, axis=-1, keepdims=True) for t in v)
            inv = lax.rsqrt(s / D + EPS)
            for k in range(R):
                dst[ahead(base + i * 16, 16, 16), k * DZ:(k + 1) * DZ] = (v[k] * inv * gain[k]).astype(BF)
            return 0
        lax.fori_loop(0, n // 16, step, 0)

    for g in s2:
        g.wait()
    nrow = c * R + x
    norm(XN, G1F, NF, nrow * B, 0, B)

    def nhalf(xx, h):
        return NF.at[span((c * R + xx) * 2 + h, H), :]

    ns, nsib = Sends(NF.at[0:7 * B, :]), [Got(NF.at[0:3 * B, :]), Got(NF.at[0:B, :])]
    xr = Ring("x", ns, NF.at[0:B, :], nhalf)

    def n_sib(xx, got):
        ref = NF.at[span(c * R + xx, B), :]
        send(ns, ref, ref, sib, got)

    ref = NF.at[span(nrow, B), :]
    xr.own(ref, ref)
    n_sib(x, nsib[0])
    z_onward(0)
    z_own(2)
    qz.wait_far()
    l_wq.wait()
    qys, qsib = Sends(WQ.at[:, 0:7]), Got(WQ.at[:, 0:R])
    slab = WQ.at[0, 0]
    qgot = [[Got(slab), Got(slab)] for _ in range(R)]
    qfar = [Got(slab) for _ in range(R)]

    def q_own(j):
        ref = WQ.at[j, blk]
        for d, g in zip((PLUS, MINUS), qgot[j]):
            send(qys, ref, ref, {"y": at("y", d)}, g)
        send(qys, ref, ref, sib, qsib)

    def q_onward(j):
        for i, (d, g) in enumerate(zip((PLUS, MINUS), qgot[j])):
            g.wait()
            ref = WQ.at[j, at("y", R - d) * 2 + c]
            if i == j // 2:
                send(qys, ref, ref, {"y": at("y", d)}, qfar[j])
            send(qys, ref, ref, sib, qsib)

    def q_last(j):
        qfar[j].wait()
        ref = WQ.at[j, at("y", FAR) * 2 + c]
        send(qys, ref, ref, sib, qsib)

    for j in (0, 2, 1):
        q_own(j)
    z_onward(1)
    z_own(3)
    xr.wait()
    xr.onward()
    n_sib(at("x", MINUS), nsib[0])
    n_sib(at("x", PLUS), nsib[0])

    og.wait()
    OS[...] = PB[:, :, x] + OR[0] + OR[1] + OR[2]
    zs2, zg2 = Sends(OD.at[0:R - 1]), [Got(OD.at[0:2]), Got(OD.at[0])]
    os2, og2 = Sends(OD.at[0, :, 0:B]), Got(OD.at[0, :, 0:B])
    os.wait()
    sends.remove(os)

    def o_send(ds, got):
        for d in ds:
            for c2 in (c, oc):
                send(zs2, OS.at[at("z", d), c2], OD.at[z, :, span(c, B)], {"z": at("z", d), "c": c2}, got)

    units = [[(0, 0, 3)], [(1, 0, 3)], [(0, 3, R), (1, 3, R)], [(2, 0, 2)], [(2, 2, R)], [(3, 0, 2)], [(3, 2, R)]]
    asend = Sends(AF.at[:, :, 0:NQ * 7 * B])
    arest = Got(AF.at[:, :, 0:NQ * 5 * B])
    agot = []
    for u in units:
        n = AF.at[0:sum(hi - lo for _, lo, hi in u), :, 0:B]
        agot.append([Got(n), Got(n)])
    NF4 = NF.reshape(2, R, B, D)

    def act(u):
        for q, lo, hi in units[u]:
            def step(s, _):
                xb = at("x", s + s // 2 - s // 3 * 2)
                gu = jnp.dot(NF4[:, xb].reshape(2 * B, D), WGU[q], preferred_element_type=F32)
                g, up = gu[:, :B], gu[:, B:]
                AL[q, :, s] = (g * lax.logistic(g) * up).astype(BF).reshape(2, B, B)
                return 0
            lax.fori_loop(lo, hi, step, 0)
            col = span(blk * NQ + q, B)
            dst = AF.at[lo:hi, :, col]
            for i, d in enumerate((PLUS, MINUS)):
                for c2 in range(2):
                    for c1 in range(2):
                        @pl.when(c == c1)
                        def _():
                            send(asend, AL.at[q, c2, lo:hi], dst, {"y": at("y", d), "c": c2}, agot[u][i] if c1 == i else arest)
            send(asend, AL.at[q, oc, lo:hi], dst, sib, arest)
            AF[lo:hi, :, col] = AL[q, c, lo:hi]

    def a_onward(u):
        for i, d in enumerate((PLUS, MINUS)):
            agot[u][i].wait()
            for q, lo, hi in units[u]:
                ref = AF.at[lo:hi, :, span((at("y", R - d) * 2 + i) * NQ + q, B)]
                send(asend, ref, ref, {"y": at("y", d)}, arest)

    nsib[0].wait()
    zr[0].wait_far()
    act(0)
    z_onward(2)
    zr[1].wait_far()
    act(1)
    xr.wait_far()
    n_sib(at("x", FAR), nsib[1])
    a_onward(0)
    nsib[1].wait()
    act(2)
    a_onward(1)
    z_onward(3)
    q_onward(0)
    q_onward(2)
    for p in range(NP):
        w_own(p)
    send(os2, OS.at[z, oc], OD.at[z, :, span(c, B)], sib, og2)
    OD[z, :, span(c, B)] = OS[z, c]
    a_onward(2)
    zr[2].wait_far()
    act(3)
    act(4)
    zr[3].wait_far()
    act(5)
    act(6)
    a_onward(3)
    a_onward(4)
    w_onward(0)
    a_onward(5)
    a_onward(6)
    q_own(3)
    q_onward(1)
    w_onward(1)
    l_wd.wait()

    zk = [z, at("z", MINUS), at("z", PLUS), at("z", FAR)]
    rsend = [Sends(RB.at[0:R - 1]), Sends(RB.at[0])]
    block = RB.at[0, 0, 0, 0:H]
    rgot = [[[Got(block), Got(block), Got(RB.at[k, 0:2, :, 0:H])] for _ in range(2)] for k in range(R - 1)]
    rlast = [[Got(RB.at[0, :, 0, 0:H]) for _ in range(2)] for _ in range(2)]
    ngot = [Got(N2.at[:, 0:H]) for _ in range(2)]
    xgot, xsend = [Got(xo.at[0:7 * B]), Got(xo.at[0:24 * B])], Sends(xo.at[0:31 * B])
    nsend = new("s")

    def halves(h):
        return slice(h * H, h * H + H)

    def product(k, h, w, kk=slice(0, D)):
        return jnp.dot(AF[:, halves(h), kk].reshape(2 * B, w.shape[0]), w, preferred_element_type=F32)

    def early(k, h):
        spans = [slice(0, D - DZ)] if k == 1 else [slice(2 * DZ, D), slice(0, DZ)]
        p = sum(product(k, h, WD[zk[k], kk], kk) for kk in spans)
        for i in range(2):
            PB[k, i, :, halves(h)] = p[:, i * B:(i + 1) * B].reshape(R, H, B)

    def down_last(i, h):
        t, k = halves(h), R - 1
        p = product(k, h, WD[zk[k], :, i * B:(i + 1) * B])
        PB[k, i, :, t] = p.reshape(R, H, B)
        for j, d in enumerate(DIST):
            if j:
                send(rsend[1], PB.at[k, i, j, t], RB.at[k, j - 1, i, t], {"x": at("x", d)}, rlast[i][h])

    def down(k, h):
        t = halves(h)
        kk = (slice(0, D), slice(D - DZ, D), slice(DZ, 2 * DZ))[k]
        p = product(k, h, WD[zk[k], kk], kk)
        for i in range(2):
            v = p[:, i * B:(i + 1) * B].reshape(R, H, B)
            PB[k, i, :, t] = PB[k, i, :, t] + v if k else v
        for i, d in enumerate((PLUS, MINUS)):
            to = {"x": at("x", d)}
            send(rsend[0], PB.at[k, i, R - 1, t], RB.at[k, R - 2, i, t], to, rgot[k][h][i])
            send(rsend[0], PB.at[k, 1 - i, 1 + i, t], RB.at[k, i, 1 - i, t], to, rgot[k][h][2])

    def add(k, h):
        t = halves(h)
        for i, d in enumerate((PLUS, MINUS)):
            rgot[k][h][i].wait()
            PB[k, i, 1 + i, t] = PB[k, i, 1 + i, t] + RB[k, R - 2, i, t]
            send(rsend[0], PB.at[k, i, 1 + i, t], RB.at[k, i, i, t], {"x": at("x", d)}, rgot[k][h][2])

    def finish(k, h, i, yy):
        t, part = halves(h), slice(i * B, (i + 1) * B)
        XP[k, t, part] = (XN[zk[k], t, span(y * 2 + i, B)].astype(F32) + (OD[zk[k], t, part] + PB[k, i, 0, t] + yy)).astype(BF)

    def resid(k, h):
        t = halves(h)
        rgot[k][h][2].wait()
        for i in range(2):
            finish(k, h, i, RB[k, 0, i, t] + RB[k, 1, i, t])

    def resid_last(i, h):
        t, k = halves(h), R - 1
        rlast[i][h].wait()
        finish(k, h, i, RB[k, 0, i, t] + RB[k, 1, i, t] + RB[k, 2, i, t])

    def tell(k, h, i=None):
        t = halves(h)
        if i is None:
            src, dst = XP.at[k, t], N2.at[zk[k], t, span(y, 2 * B)]
        else:
            src, dst = XP.at[k, t, i * B:(i + 1) * B], N2.at[zk[k], t, span(y * 2 + i, B)]
        for d in range(R):
            cp = pltpu.make_async_remote_copy(
                src_ref=src, dst_ref=dst, send_sem=ss.at[nsend], recv_sem=rs.at[ngot[h].i],
                device_id={"x": at("x", d), "y": x}, device_id_type=MESH)
            if d:
                cp.start()
            else:
                pl.when(x != y)(cp.start)

                @pl.when(x == y)
                def _():
                    dst[...] = src[...]

    def x_out(k):
        rows = xo.at[span((z * 2 + c) * R + x, B), :]
        send(xsend, XP.at[k, :, span(oc, B)], rows, {"z": zk[k], "c": oc}, xgot[0])
        if k:
            send(xsend, XP.at[k, :, span(c, B)], rows, {"z": zk[k]}, xgot[0])
        else:
            rows[...] = XP[k, :, span(c, B)]

    def x_onward():
        xgot[0].wait()
        ref = xo.reshape(R, 2, R, B, B).at[:, :, x]
        for d in (PLUS, MINUS, FAR):
            send(xsend, ref, ref, {"x": at("x", d)}, xgot[1])

    arest.wait()
    wsib.wait()
    down(0, 0)
    down(0, 1)
    w_near(0, range(2))
    w_near(1, range(2))
    for lane in range(2):
        w_far(0, lane)
        w_far(1, lane)
    o_send((PLUS, MINUS), zg2[0])
    o_send((FAR,), zg2[1])
    w_onward(2)
    w_near(0, (2,))
    early(1, 0)
    w_onward(3)
    early(1, 1)
    add(0, 0)
    w_near(0, (NP - 1,))
    down(1, 0)
    w_near(1, (2, NP - 1))
    down(1, 1)
    add(0, 1)
    early(2, 0)
    down(2, 0)
    early(2, 1)
    down(2, 1)
    add(1, 0)
    add(1, 1)
    og2.wait()
    resid(0, 0)
    tell(0, 0)
    resid(0, 1)
    x_out(0)
    q_onward(3)
    q_last(0)
    q_last(2)
    add(2, 0)
    add(2, 1)
    tell(0, 1)
    far(0)
    wlast[0].wait()
    down_last(0, 0)
    down_last(0, 1)
    far(1)
    wlast[1].wait()
    down_last(1, 0)
    down_last(1, 1)
    zg2[0].wait()
    for k in (1, 2):
        resid(k, 0)
        tell(k, 0)
    for k in (1, 2):
        resid(k, 1)
        x_out(k)
    zg2[1].wait()
    resid_last(0, 0)
    tell(3, 0, 0)
    resid_last(0, 1)
    q_last(1)
    q_last(3)
    resid_last(1, 0)
    tell(3, 0, 1)
    tell(1, 1)
    tell(2, 1)
    tell(3, 1, 0)
    resid_last(1, 1)
    tell(3, 1, 1)
    x_out(3)
    qsib.wait()

    def qrow(zz, yy, off, n):
        return qo.at[ahead(((zz * 2 + c) * R + yy) * B + off, n, Q), :]

    osend, osib = Sends(qo.at[0:31 * B]), Got(qo.at[0:D // 2])

    def qkv(h):
        t = halves(h)

        @pl.when(x == y)
        def _():
            ngot[h].wait(N2.at[:, 0:H, 0:6 * B])

        @pl.when(x != y)
        def _():
            ngot[h].wait()
        norm(N2, G2F, N2B, h * H, h * H, H)
        for j in range(3):
            cols = slice(j * 3 * B, (j + 1) * 3 * B)
            w = WQ[:, :, :, cols].reshape(D, 3 * B)
            qo[ahead(((z * 2 + c) * R + y) * B + h * H, H, H), cols] = jnp.dot(
                N2B[t, :], w, preferred_element_type=F32).astype(BF)
            fan[h](cols)

    def out_sib(ref):
        send(osend, ref, ref, sib, osib)

    todo = {}

    def coming(name, ref, then, whole):
        todo[name] = (Got(ref), then, whole)

    def arrivals(h):
        first, second = "yz" if h == 0 else "zy"

        def block(i, j, off, n):
            a, b = at(first, i), at(second, j)
            return qrow(b if h == 0 else a, a if h == 0 else b, h * H + off, n)

        def hop(axis, d, ref, name):
            send(osend, ref, ref, {axis: at(axis, d)}, todo[name][0])

        def across(name, i, parts):
            def start():
                for off, n, part in parts:
                    for d in (PLUS, MINUS):
                        hop(second, d, block(i, 0, off, n), f"s{h}{name}{part}{d}")
            for off, n, part in parts:
                for u, d in enumerate((PLUS, MINUS)):
                    def onward(u=u, d=d, off=off, part=part):
                        if part in ("", str(u)):
                            hop(second, d, block(i, R - d, u * Q, Q), f"l{h}{name}{u}")
                    coming(f"s{h}{name}{part}{d}", block(i, R - d, off, n), onward, block(i, R - d, off, n))
            for u in range(2):
                ref = block(i, FAR, u * Q, Q)
                coming(f"l{h}{name}{u}", ref, None, ref)
            return start

        full = [(0, H, "")]
        go = {name: across(name, i, full) for name, i in (("o", 0), ("m", MINUS), ("p", PLUS))}
        across("f", FAR, [(0, Q, "0"), (Q, Q, "1")])
        for u, (d, name) in enumerate(((PLUS, "m"), (MINUS, "p"))):
            def onward(u=u, d=d, name=name):
                hop(first, d, block(R - d, 0, u * Q, Q), f"r{h}{u}")
                go[name]()
            coming(f"f{h}{d}", block(R - d, 0, 0, H), onward, block(R - d, 0, 0, H))
            ref = block(FAR, 0, u * Q, Q)

            def rest(u=u):
                for d in (PLUS, MINUS):
                    hop(second, d, block(FAR, 0, u * Q, Q), f"s{h}f{u}{d}")
            coming(f"r{h}{u}", ref, rest, ref)

        def own(cols):
            ref = block(0, 0, 0, H).at[:, cols]
            for d in (PLUS, MINUS):
                hop(first, d, ref, f"f{h}{d}")
            for d in (PLUS, MINUS):
                hop(second, d, ref, f"s{h}o{d}")
            out_sib(ref)
        return own

    fan = [arrivals(h) for h in range(2)]
    for h in range(2):
        qkv(h)
    x_onward()
    for key in ("f0", "s0o", "s1o", "f1", "r0", "s0m", "l1o", "s0p", "s1m", "l0o", "r1", "s1p",
                "s0f0", "l1m", "s0f1", "s1f0", "l0m", "s1f1", "l0p", "l1p", "l0f", "l1f"):
        for name in [n for n in todo if n.startswith(key)]:
            got, then, ref = todo.pop(name)
            got.wait()
            if then:
                then()
            out_sib(ref)
    assert not todo
    osib.wait()
    xgot[1].wait()
    for s in sends:
        s.wait()

    @pl.when(x == y)
    def _():
        r = N2.at[:, :, 0:6 * B]
        pltpu.make_async_copy(r, r, ss.at[nsend]).wait()

    @pl.when(x != y)
    def _():
        pltpu.make_async_copy(N2, N2, ss.at[nsend]).wait()


def _copy(a, b, c, d, sem):
    n = 4
    cps = []
    for i, (src, dst) in enumerate(((a, c), (b, d))):
        for j in range(n):
            r = slice(j * D // n, (j + 1) * D // n)
            cps.append(pltpu.make_async_copy(src.at[r], dst.at[r], sem.at[i, j]))
            cps[-1].start()
    for cp in cps:
        cp.wait()


def solution(mesh):
    mesh4 = Mesh(mesh.devices.reshape(R, R, R, 2), ("x", "z", "y", "c"))

    def body(x, g1, g2, w_gate, w_up, w_down, o, w_o, w_qkv):
        vm = pltpu.VMEM
        anyspec = pl.BlockSpec(memory_space=pl.ANY)
        sem = pltpu.SemaphoreType.DMA
        outs = pl.pallas_call(
            _kernel,
            out_shape=(vm((D, B), BF), vm((D, W), BF)),
            in_specs=[anyspec] * 9,
            out_specs=(pl.BlockSpec(memory_space=vm), pl.BlockSpec(memory_space=vm)),
            scratch_shapes=[
                vm((R, 2, B, B), BF),
                vm((R, B, DZ), BF),
                vm((R, 1, B), F32), vm((R, 1, B), F32),
                vm((R, 1, DZ), F32), vm((R, 1, DZ), F32),
                vm((DZ, D), BF),
                vm((NQ, D, 2 * B), BF),
                vm((NQ, 2, R, B, B), BF),
                vm((R, B, D), BF),
                vm((R, 2 * B, DZ), BF),
                vm((DZ, B), BF),
                vm((R - 1, R, 2, B, B), F32),
                vm((R, 2, B, B), F32),
                vm((R, B, 2 * B), F32),
                vm((R, D, 2 * B), BF),
                vm((R, 2, R, B, B), F32),
                vm((R, R - 1, 2, B, B), F32),
                vm((R, B, 2 * B), BF),
                vm((R, B, DZ), BF),
                vm((B, D), BF),
                vm((R, 8, B, W), BF),
                sem((NSEND,)), sem((NRECV,)), sem((NLOC,)),
            ],
            compiler_params=pltpu.CompilerParams(
                collective_id=0, has_side_effects=True, vmem_limit_bytes=53 * 2**20),
            name="block",
        )(x.reshape(R, 2, R, B, B), g1.reshape(1, B), g2.reshape(1, B), w_gate, w_up, w_down, o, w_o, w_qkv)
        return pl.pallas_call(
            _copy,
            out_shape=(jax.ShapeDtypeStruct((D, B), BF), jax.ShapeDtypeStruct((D, W), BF)),
            in_specs=[pl.BlockSpec(memory_space=vm)] * 2,
            out_specs=(anyspec, anyspec),
            scratch_shapes=[sem((2, 4))],
            compiler_params=pltpu.CompilerParams(vmem_limit_bytes=2**20),
            name="store",
        )(*outs)

    h = ("z", "y", "c")
    in_specs = (P(None, h), P(h), P(h), P(h, "x"), P(h, "x"), P("x", h), P(None, "x"), P("x", h), P(h, "x"))
    return jax.shard_map(body, mesh=mesh4, in_specs=in_specs, out_specs=(P(None, h), P(None, "x")), check_vma=False)
```

```python
import jax
import jax.numpy as jnp
from jax import lax
from jax.experimental import pallas as pl
from jax.experimental.pallas import tpu as pltpu
from jax.sharding import Mesh, PartitionSpec as P

EPS = 1e-6
MESH = pl.DeviceIdType.MESH
BF = jnp.bfloat16
F32 = jnp.float32
R = 4
B = 128
H = B // 2
Q = H // 2
D = 4096
DZ = D // R
DC = DZ // 2
NQ = 4
NP = 4
W = 1152
NSEND, NRECV, NLOC = 21, 156, 19


def _kernel(x5, g1, g2, wg, wu, wd, o, wo, wq, xo, qo,
            XR, XN, G1S, G2S, G1F, G2F, NF, WGU, AL, AF, OT, WO, OR, OS, OD, WD, PB, RB, XP, N2, N2B, WQ,
            ss, rs, ls):
    x, y, z, c = (lax.axis_index(a) for a in "xyzc")
    here = {"x": x, "y": y, "z": z}

    def at(axis, d):
        return lax.rem(here[axis] + d, R)

    PLUS, MINUS, FAR = 1, R - 1, 2
    oc = 1 - c
    sib = {"c": oc}
    blk = y * 2 + c

    count = {"s": 0, "r": 0, "l": 0}
    limit = {"s": NSEND, "r": NRECV, "l": NLOC}

    def new(kind):
        count[kind] += 1
        assert count[kind] <= limit[kind]
        return count[kind] - 1

    sends = []

    class Sends:
        def __init__(self, ref):
            self.i, self.ref = new("s"), ref
            sends.append(self)

        def wait(self):
            pltpu.make_async_copy(self.ref, self.ref, ss.at[self.i]).wait()

    class Got:
        def __init__(self, ref):
            self.i, self.ref = new("r"), ref

        def wait(self, ref=None):
            ref = self.ref if ref is None else ref
            pltpu.make_async_copy(ref, ref, rs.at[self.i]).wait()

    def send(group, src, dst, dev, got):
        d = pltpu.make_async_remote_copy(
            src_ref=src, dst_ref=dst, send_sem=ss.at[group.i], recv_sem=rs.at[got.i],
            device_id=dev, device_id_type=MESH)
        d.start()

    def here_copy(src, dst, got):
        pltpu.make_async_copy(src, dst, rs.at[got.i]).start()

    def load(src, dst):
        d = pltpu.make_async_copy(src, dst, ls.at[new("l")])
        d.start()
        return d

    def span(b, n):
        return pl.ds(pl.multiple_of(b * n, n), n)

    def ahead(b, n, step):
        return pl.ds(pl.multiple_of(b, step), n)

    bar = pltpu.get_barrier_semaphore()
    peers = [(dx, 0, 0, 0) for dx in range(1, R)]
    peers += [(0, dy, 0, dc) for dy in range(R) for dc in range(2) if dy + dc]
    peers += [(0, 0, dz, dc) for dz in range(1, R) for dc in range(2)]
    for dx, dy, dz, dc in peers:
        pl.semaphore_signal(bar, inc=1, device_id={
            "x": at("x", dx), "y": at("y", dy), "z": at("z", dz), "c": oc if dc else c}, device_id_type=MESH)

    DIST = (0, PLUS, MINUS, FAR)
    l_wo = load(wo, WO)
    NT = D // (2 * B)
    tiles = [pltpu.make_async_copy(o.at[i * 2 * B:(i + 1) * 2 * B, :], OT.at[i % R], ls.at[new("l")]) for i in range(NT)]
    for i in range(R):
        tiles[i].start()
    l_wd = load(wd, WD.at[z, :, span(c, B)])
    l_wq = load(wq, WQ.at[z, blk])
    pl.semaphore_wait(bar, len(peers))

    near = [(dy, dc) for dy in (PLUS, MINUS, FAR, 0) for dc in range(2) if dy + dc]

    def yc(dy, dc):
        return at("y", dy), (oc if dc else c)

    firsts = ((x5, XR, XN), (g1, G1S, G1F), (g2, G2S, G2F))
    s1, s1s = [Got(b) for _, b, _ in firsts], [Sends(b.at[0:R - 1]) for _, b, _ in firsts]
    for dz in (PLUS, MINUS, FAR, 0):
        z2 = at("z", dz)
        for (src, dst, _), got, grp in zip(firsts, s1, s1s):
            s = src.at[z2, :, x] if src is x5 else src
            if dz:
                send(grp, s, dst.at[z], {"z": z2}, got)
            else:
                here_copy(s, dst.at[z], got)

    a2a, a2as = [Got(WGU.at[q, span(z, DZ), :]) for q in range(NQ)], Sends(NF.at[0:NQ * 7 * 8, :])

    def send_a2a(q):
        r = span(z * 8 + blk, B)
        for dy, dc in near + [(0, 0)]:
            y2, c2 = yc(dy, dc)
            cols = span((y2 * 2 + c2) * NQ + q, B)
            for w, off in ((wg, 0), (wu, B)):
                s, d = w.at[:, cols], WGU.at[q, r, off:off + B]
                if dy + dc:
                    send(a2as, s, d, {"y": y2, "c": c2}, a2a[q])
                else:
                    here_copy(s, d, a2a[q])

    class Ring:
        def __init__(self, axis, sends, own, half):
            self.axis, self.sends, self.half = axis, sends, half
            self.got = [Got(own), Got(own)]
            self.far = Got(own)

        def own(self, src, dst):
            for d, g in zip((PLUS, MINUS), self.got):
                send(self.sends, src, dst, {self.axis: at(self.axis, d)}, g)

        def wait(self):
            for g in self.got:
                g.wait()

        def onward(self):
            for h, d in enumerate((PLUS, MINUS)):
                ref = self.half(at(self.axis, R - d), h)
                send(self.sends, ref, ref, {self.axis: at(self.axis, d)}, self.far)

        def wait_far(self):
            self.far.wait()

    send_a2a(0)
    send_a2a(1)
    qz = Ring("z", Sends(WQ.at[0, 0:R - 1]), WQ.at[0, 0], lambda zz, h: WQ.at[zz, blk, h * H:h * H + H])
    qz.own(wq, WQ.at[z, blk])

    wds = Sends(WD.at[:, 0:D * 7 // 8, :])
    cuts = [(p, p * DZ, (p + 1) * DZ) for p in range(NP)]
    wgot = [[Got(WD.at[0, s:e, 0:B]), Got(WD.at[0, s:e, 0:B])] for _, s, e in cuts]
    piece = WD.at[0, 0:DZ, 0:B]
    wsib, wnear = Got(WD.at[0, :, 0:B]), [[Got(piece), Got(piece)] for _ in range(NP)]
    wfar, wlast = [[Got(piece), Got(piece)] for _ in range(2)], [Got(WD.at[0, 0:2 * DZ, 0:B]) for _ in range(2)]

    def cut(i, h):
        p = (i + 2 * h) % NP
        return cuts[p]

    def w_own(i):
        for h, (d, g) in enumerate(zip((PLUS, MINUS), wgot[i])):
            _, s, e = cut(i, h)
            send(wds, wd.at[s:e, :], WD.at[z, s:e, span(c, B)], {"z": at("z", d)}, g)
        _, s, e = cuts[i]
        send(wds, wd.at[s:e, :], WD.at[z, s:e, span(c, B)], sib, wsib)

    def w_onward(i):
        for h, (d, g) in enumerate(zip((PLUS, MINUS), wgot[i])):
            g.wait()
            _, s, e = cut(i, h)
            ref = WD.at[at("z", R - d), s:e, span(c, B)]
            send(wds, ref, ref, sib, wnear[i][h])

    def w_near(h, ps):
        for p in ps:
            wnear[p][h].wait()

    def w_far(h, lane):
        d = (PLUS, MINUS)[h]
        ref = WD.at[at("z", R - d), span(2 * h + c, DZ), lane * B:(lane + 1) * B]
        send(wds, ref, ref, {"z": at("z", d)}, wfar[lane][h])

    def far(lane):
        for h, g in enumerate(wfar[lane]):
            g.wait()
            ref = WD.at[at("z", FAR), span(2 * h + c, DZ), lane * B:(lane + 1) * B]
            send(wds, ref, ref, sib, wlast[lane])

    l_wo.wait()
    os, og = Sends(OR), Got(OR)
    for i in range(NT):
        tiles[i].wait()
        p, q, r = i // 2 // 2, i // 2 % 2, i % 2 * 2
        PB[p, q, r:r + 2] = jnp.dot(OT[i % R], WO[...], preferred_element_type=F32).reshape(2, B, B)
        if i + R < NT:
            tiles[i + R].start()
        if q and r:
            for j, d in enumerate((PLUS, MINUS, FAR)):
                send(os, PB.at[p, :, at("x", d)], OR.at[j, p], {"x": at("x", d)}, og)
    for g in s1:
        g.wait()
    less = slice(0, 7 * B)
    s2, s2s = [Got(b.at[:, :, less]) for _, _, b in firsts], [Sends(b.at[:, :, less]) for _, _, b in firsts]
    for dy, dc in near:
        y2, c2 = yc(dy, dc)
        for (_, src, dst), got, grp in zip(firsts, s2, s2s):
            send(grp, src.at[:, c2] if src is XR else src, dst.at[:, :, span(blk, B)], {"y": y2, "c": c2}, got)
    for q in range(2, NQ):
        send_a2a(q)
    XN[:, :, span(blk, B)] = XR[:, c]
    G1F[:, :, span(blk, B)] = G1S[...]
    G2F[:, :, span(blk, B)] = G2S[...]

    zs = Sends(NF.at[0:NQ * R * (R - 1) * 16, :])
    zr = [Ring("z", zs, WGU.at[q, 0:DZ, :],
               lambda zz, h, q=q: WGU.at[q, span(zz * 2 + h, DC), :]) for q in range(NQ)]

    def z_own(q):
        a2a[q].wait()
        ref = WGU.at[q, span(z, DZ), :]
        zr[q].own(ref, ref)

    def z_onward(q):
        zr[q].wait()
        zr[q].onward()

    z_own(0)
    z_own(1)
    qz.wait()
    qz.onward()

    def norm(src, gain, dst, base, first, n):
        def step(i, _):
            r = span(first // 16 + i, 16)
            v = [src[k, r, :].astype(F32) for k in range(R)]
            s = sum(jnp.sum(t * t, axis=-1, keepdims=True) for t in v)
            inv = lax.rsqrt(s / D + EPS)
            for k in range(R):
                dst[ahead(base + i * 16, 16, 16), k * DZ:(k + 1) * DZ] = (v[k] * inv * gain[k]).astype(BF)
            return 0
        lax.fori_loop(0, n // 16, step, 0)

    for g in s2:
        g.wait()
    nrow = c * R + x
    norm(XN, G1F, NF, nrow * B, 0, B)

    def nhalf(xx, h):
        return NF.at[span((c * R + xx) * 2 + h, H), :]

    ns, nsib = Sends(NF.at[0:7 * B, :]), [Got(NF.at[0:3 * B, :]), Got(NF.at[0:B, :])]
    xr = Ring("x", ns, NF.at[0:B, :], nhalf)

    def n_sib(xx, got):
        ref = NF.at[span(c * R + xx, B), :]
        send(ns, ref, ref, sib, got)

    ref = NF.at[span(nrow, B), :]
    xr.own(ref, ref)
    n_sib(x, nsib[0])
    z_onward(0)
    z_own(2)
    qz.wait_far()
    l_wq.wait()
    qys, qsib = Sends(WQ.at[:, 0:7]), Got(WQ.at[:, 0:R])
    slab = WQ.at[0, 0]
    qgot = [[Got(slab), Got(slab)] for _ in range(R)]
    qfar = [Got(slab) for _ in range(R)]

    def q_own(j):
        ref = WQ.at[j, blk]
        for d, g in zip((PLUS, MINUS), qgot[j]):
            send(qys, ref, ref, {"y": at("y", d)}, g)
        send(qys, ref, ref, sib, qsib)

    def q_onward(j):
        for i, (d, g) in enumerate(zip((PLUS, MINUS), qgot[j])):
            g.wait()
            ref = WQ.at[j, at("y", R - d) * 2 + c]
            if i == j // 2:
                send(qys, ref, ref, {"y": at("y", d)}, qfar[j])
            send(qys, ref, ref, sib, qsib)

    def q_last(j):
        qfar[j].wait()
        ref = WQ.at[j, at("y", FAR) * 2 + c]
        send(qys, ref, ref, sib, qsib)

    for j in (0, 2, 1):
        q_own(j)
    z_onward(1)
    z_own(3)
    xr.wait()
    xr.onward()
    n_sib(at("x", MINUS), nsib[0])
    n_sib(at("x", PLUS), nsib[0])

    og.wait()
    OS[...] = PB[:, :, x] + OR[0] + OR[1] + OR[2]
    zs2, zg2 = Sends(OD.at[0:R - 1]), [Got(OD.at[0:2]), Got(OD.at[0])]
    os2, og2 = Sends(OD.at[0, :, 0:B]), Got(OD.at[0, :, 0:B])
    os.wait()
    sends.remove(os)

    def o_send(ds, got):
        for d in ds:
            for c2 in (c, oc):
                send(zs2, OS.at[at("z", d), c2], OD.at[z, :, span(c, B)], {"z": at("z", d), "c": c2}, got)

    units = [[(0, 0, 3)], [(1, 0, 3)], [(0, 3, R), (1, 3, R)], [(2, 0, 2)], [(2, 2, R)], [(3, 0, 2)], [(3, 2, R)]]
    asend = Sends(AF.at[:, :, 0:NQ * 7 * B])
    arest = Got(AF.at[:, :, 0:NQ * 5 * B])
    agot = []
    for u in units:
        n = AF.at[0:sum(hi - lo for _, lo, hi in u), :, 0:B]
        agot.append([Got(n), Got(n)])
    NF4 = NF.reshape(2, R, B, D)

    def act(u):
        for q, lo, hi in units[u]:
            def step(s, _):
                xb = at("x", s + s // 2 - s // 3 * 2)
                gu = jnp.dot(NF4[:, xb].reshape(2 * B, D), WGU[q], preferred_element_type=F32)
                g, up = gu[:, :B], gu[:, B:]
                AL[q, :, s] = (g * lax.logistic(g) * up).astype(BF).reshape(2, B, B)
                return 0
            lax.fori_loop(lo, hi, step, 0)
            col = span(blk * NQ + q, B)
            dst = AF.at[lo:hi, :, col]
            for i, d in enumerate((PLUS, MINUS)):
                for c2 in range(2):
                    for c1 in range(2):
                        @pl.when(c == c1)
                        def _():
                            send(asend, AL.at[q, c2, lo:hi], dst, {"y": at("y", d), "c": c2}, agot[u][i] if c1 == i else arest)
            send(asend, AL.at[q, oc, lo:hi], dst, sib, arest)
            AF[lo:hi, :, col] = AL[q, c, lo:hi]

    def a_onward(u):
        for i, d in enumerate((PLUS, MINUS)):
            agot[u][i].wait()
            for q, lo, hi in units[u]:
                ref = AF.at[lo:hi, :, span((at("y", R - d) * 2 + i) * NQ + q, B)]
                send(asend, ref, ref, {"y": at("y", d)}, arest)

    nsib[0].wait()
    zr[0].wait_far()
    act(0)
    z_onward(2)
    zr[1].wait_far()
    act(1)
    xr.wait_far()
    n_sib(at("x", FAR), nsib[1])
    a_onward(0)
    nsib[1].wait()
    act(2)
    a_onward(1)
    z_onward(3)
    q_onward(0)
    q_onward(2)
    for p in range(NP):
        w_own(p)
    send(os2, OS.at[z, oc], OD.at[z, :, span(c, B)], sib, og2)
    OD[z, :, span(c, B)] = OS[z, c]
    a_onward(2)
    zr[2].wait_far()
    act(3)
    act(4)
    zr[3].wait_far()
    act(5)
    act(6)
    a_onward(3)
    a_onward(4)
    w_onward(0)
    a_onward(5)
    a_onward(6)
    q_own(3)
    q_onward(1)
    w_onward(1)
    l_wd.wait()

    zk = [z, at("z", MINUS), at("z", PLUS), at("z", FAR)]
    rsend = [Sends(RB.at[0:R - 1]), Sends(RB.at[0])]
    block = RB.at[0, 0, 0, 0:H]
    rgot = [[[Got(block), Got(block), Got(RB.at[k, 0:2, :, 0:H])] for _ in range(2)] for k in range(R - 1)]
    rlast = [[Got(RB.at[0, :, 0, 0:H]) for _ in range(2)] for _ in range(2)]
    ngot = [Got(N2.at[:, 0:H]) for _ in range(2)]
    xgot, xsend = [Got(xo.at[0:7 * B]), Got(xo.at[0:24 * B])], Sends(xo.at[0:31 * B])
    nsend = new("s")

    def halves(h):
        return slice(h * H, h * H + H)

    def product(k, h, w, kk=slice(0, D)):
        return jnp.dot(AF[:, halves(h), kk].reshape(2 * B, w.shape[0]), w, preferred_element_type=F32)

    def early(k, h):
        spans = [slice(0, D - DZ)] if k == 1 else [slice(2 * DZ, D), slice(0, DZ)]
        p = sum(product(k, h, WD[zk[k], kk], kk) for kk in spans)
        for i in range(2):
            PB[k, i, :, halves(h)] = p[:, i * B:(i + 1) * B].reshape(R, H, B)

    def down_last(i, h):
        t, k = halves(h), R - 1
        p = product(k, h, WD[zk[k], :, i * B:(i + 1) * B])
        PB[k, i, :, t] = p.reshape(R, H, B)
        for j, d in enumerate(DIST):
            if j:
                send(rsend[1], PB.at[k, i, j, t], RB.at[k, j - 1, i, t], {"x": at("x", d)}, rlast[i][h])

    def down(k, h):
        t = halves(h)
        kk = (slice(0, D), slice(D - DZ, D), slice(DZ, 2 * DZ))[k]
        p = product(k, h, WD[zk[k], kk], kk)
        for i in range(2):
            v = p[:, i * B:(i + 1) * B].reshape(R, H, B)
            PB[k, i, :, t] = PB[k, i, :, t] + v if k else v
        for i, d in enumerate((PLUS, MINUS)):
            to = {"x": at("x", d)}
            send(rsend[0], PB.at[k, i, R - 1, t], RB.at[k, R - 2, i, t], to, rgot[k][h][i])
            send(rsend[0], PB.at[k, 1 - i, 1 + i, t], RB.at[k, i, 1 - i, t], to, rgot[k][h][2])

    def add(k, h):
        t = halves(h)
        for i, d in enumerate((PLUS, MINUS)):
            rgot[k][h][i].wait()
            PB[k, i, 1 + i, t] = PB[k, i, 1 + i, t] + RB[k, R - 2, i, t]
            send(rsend[0], PB.at[k, i, 1 + i, t], RB.at[k, i, i, t], {"x": at("x", d)}, rgot[k][h][2])

    def finish(k, h, i, yy):
        t, part = halves(h), slice(i * B, (i + 1) * B)
        XP[k, t, part] = (XN[zk[k], t, span(y * 2 + i, B)].astype(F32) + (OD[zk[k], t, part] + PB[k, i, 0, t] + yy)).astype(BF)

    def resid(k, h):
        t = halves(h)
        rgot[k][h][2].wait()
        for i in range(2):
            finish(k, h, i, RB[k, 0, i, t] + RB[k, 1, i, t])

    def resid_last(i, h):
        t, k = halves(h), R - 1
        rlast[i][h].wait()
        finish(k, h, i, RB[k, 0, i, t] + RB[k, 1, i, t] + RB[k, 2, i, t])

    def tell(k, h, i=None):
        t = halves(h)
        if i is None:
            src, dst = XP.at[k, t], N2.at[zk[k], t, span(y, 2 * B)]
        else:
            src, dst = XP.at[k, t, i * B:(i + 1) * B], N2.at[zk[k], t, span(y * 2 + i, B)]
        for d in range(R):
            cp = pltpu.make_async_remote_copy(
                src_ref=src, dst_ref=dst, send_sem=ss.at[nsend], recv_sem=rs.at[ngot[h].i],
                device_id={"x": at("x", d), "y": x}, device_id_type=MESH)
            if d:
                cp.start()
            else:
                pl.when(x != y)(cp.start)

                @pl.when(x == y)
                def _():
                    dst[...] = src[...]

    def x_out(k):
        rows = xo.at[span((z * 2 + c) * R + x, B), :]
        send(xsend, XP.at[k, :, span(oc, B)], rows, {"z": zk[k], "c": oc}, xgot[0])
        if k:
            send(xsend, XP.at[k, :, span(c, B)], rows, {"z": zk[k]}, xgot[0])
        else:
            rows[...] = XP[k, :, span(c, B)]

    def x_onward():
        xgot[0].wait()
        ref = xo.reshape(R, 2, R, B, B).at[:, :, x]
        for d in (PLUS, MINUS, FAR):
            send(xsend, ref, ref, {"x": at("x", d)}, xgot[1])

    arest.wait()
    wsib.wait()
    down(0, 0)
    down(0, 1)
    w_near(0, range(2))
    w_near(1, range(2))
    for lane in range(2):
        w_far(0, lane)
        w_far(1, lane)
    o_send((PLUS, MINUS), zg2[0])
    o_send((FAR,), zg2[1])
    w_onward(2)
    w_near(0, (2,))
    early(1, 0)
    w_onward(3)
    early(1, 1)
    add(0, 0)
    w_near(0, (NP - 1,))
    down(1, 0)
    w_near(1, (2, NP - 1))
    down(1, 1)
    add(0, 1)
    early(2, 0)
    down(2, 0)
    early(2, 1)
    down(2, 1)
    add(1, 0)
    add(1, 1)
    og2.wait()
    resid(0, 0)
    tell(0, 0)
    resid(0, 1)
    x_out(0)
    q_onward(3)
    q_last(0)
    q_last(2)
    add(2, 0)
    add(2, 1)
    tell(0, 1)
    far(0)
    wlast[0].wait()
    down_last(0, 0)
    down_last(0, 1)
    far(1)
    wlast[1].wait()
    down_last(1, 0)
    down_last(1, 1)
    zg2[0].wait()
    for k in (1, 2):
        resid(k, 0)
        tell(k, 0)
    zg2[1].wait()
    resid_last(0, 0)
    tell(3, 0, 0)
    for k in (1, 2):
        resid(k, 1)
        x_out(k)
    resid_last(0, 1)
    q_last(1)
    q_last(3)
    resid_last(1, 0)
    tell(3, 0, 1)
    tell(1, 1)
    tell(2, 1)
    tell(3, 1, 0)
    resid_last(1, 1)
    tell(3, 1, 1)
    x_out(3)
    qsib.wait()

    def qrow(zz, yy, off, n):
        return qo.at[ahead(((zz * 2 + c) * R + yy) * B + off, n, Q), :]

    osend, osib = Sends(qo.at[0:31 * B]), Got(qo.at[0:D // 2])

    def qkv(h):
        t = halves(h)

        @pl.when(x == y)
        def _():
            ngot[h].wait(N2.at[:, 0:H, 0:6 * B])

        @pl.when(x != y)
        def _():
            ngot[h].wait()
        norm(N2, G2F, N2B, h * H, h * H, H)
        for j in range(3):
            cols = slice(j * 3 * B, (j + 1) * 3 * B)
            w = WQ[:, :, :, cols].reshape(D, 3 * B)
            qo[ahead(((z * 2 + c) * R + y) * B + h * H, H, H), cols] = jnp.dot(
                N2B[t, :], w, preferred_element_type=F32).astype(BF)
            fan[h](cols)

    def out_sib(ref):
        send(osend, ref, ref, sib, osib)

    todo = {}

    def coming(name, ref, then, whole):
        todo[name] = (Got(ref), then, whole)

    def arrivals(h):
        first, second = "yz" if h == 0 else "zy"

        def block(i, j, off, n):
            a, b = at(first, i), at(second, j)
            return qrow(b if h == 0 else a, a if h == 0 else b, h * H + off, n)

        def hop(axis, d, ref, name):
            send(osend, ref, ref, {axis: at(axis, d)}, todo[name][0])

        def across(name, i, parts):
            def start():
                for off, n, part in parts:
                    for d in (PLUS, MINUS):
                        hop(second, d, block(i, 0, off, n), f"s{h}{name}{part}{d}")
            for off, n, part in parts:
                for u, d in enumerate((PLUS, MINUS)):
                    def onward(u=u, d=d, off=off, part=part):
                        if part in ("", str(u)):
                            hop(second, d, block(i, R - d, u * Q, Q), f"l{h}{name}{u}")
                    coming(f"s{h}{name}{part}{d}", block(i, R - d, off, n), onward, block(i, R - d, off, n))
            for u in range(2):
                ref = block(i, FAR, u * Q, Q)
                coming(f"l{h}{name}{u}", ref, None, ref)
            return start

        full = [(0, H, "")]
        go = {name: across(name, i, full) for name, i in (("o", 0), ("m", MINUS), ("p", PLUS))}
        across("f", FAR, [(0, Q, "0"), (Q, Q, "1")])
        for u, (d, name) in enumerate(((PLUS, "m"), (MINUS, "p"))):
            def onward(u=u, d=d, name=name):
                hop(first, d, block(R - d, 0, u * Q, Q), f"r{h}{u}")
                go[name]()
            coming(f"f{h}{d}", block(R - d, 0, 0, H), onward, block(R - d, 0, 0, H))
            ref = block(FAR, 0, u * Q, Q)

            def rest(u=u):
                for d in (PLUS, MINUS):
                    hop(second, d, block(FAR, 0, u * Q, Q), f"s{h}f{u}{d}")
            coming(f"r{h}{u}", ref, rest, ref)

        def own(cols):
            ref = block(0, 0, 0, H).at[:, cols]
            for d in (PLUS, MINUS):
                hop(first, d, ref, f"f{h}{d}")
            for d in (PLUS, MINUS):
                hop(second, d, ref, f"s{h}o{d}")
            out_sib(ref)
        return own

    fan = [arrivals(h) for h in range(2)]
    for h in range(2):
        qkv(h)
    x_onward()
    for key in ("f0", "s0o", "s1o", "f1", "r0", "s0m", "l1o", "s0p", "s1m", "l0o", "r1", "s1p",
                "s0f0", "l1m", "s0f1", "s1f0", "l0m", "s1f1", "l0p", "l1p", "l0f", "l1f"):
        for name in [n for n in todo if n.startswith(key)]:
            got, then, ref = todo.pop(name)
            got.wait()
            if then:
                then()
            out_sib(ref)
    assert not todo
    osib.wait()
    xgot[1].wait()
    for s in sends:
        s.wait()

    @pl.when(x == y)
    def _():
        r = N2.at[:, :, 0:6 * B]
        pltpu.make_async_copy(r, r, ss.at[nsend]).wait()

    @pl.when(x != y)
    def _():
        pltpu.make_async_copy(N2, N2, ss.at[nsend]).wait()


def _copy(a, b, c, d, sem):
    n = 4
    cps = []
    for i, (src, dst) in enumerate(((a, c), (b, d))):
        for j in range(n):
            r = slice(j * D // n, (j + 1) * D // n)
            cps.append(pltpu.make_async_copy(src.at[r], dst.at[r], sem.at[i, j]))
            cps[-1].start()
    for cp in cps:
        cp.wait()


def solution(mesh):
    mesh4 = Mesh(mesh.devices.reshape(R, R, R, 2), ("x", "z", "y", "c"))

    def body(x, g1, g2, w_gate, w_up, w_down, o, w_o, w_qkv):
        vm = pltpu.VMEM
        anyspec = pl.BlockSpec(memory_space=pl.ANY)
        sem = pltpu.SemaphoreType.DMA
        outs = pl.pallas_call(
            _kernel,
            out_shape=(vm((D, B), BF), vm((D, W), BF)),
            in_specs=[anyspec] * 9,
            out_specs=(pl.BlockSpec(memory_space=vm), pl.BlockSpec(memory_space=vm)),
            scratch_shapes=[
                vm((R, 2, B, B), BF),
                vm((R, B, DZ), BF),
                vm((R, 1, B), F32), vm((R, 1, B), F32),
                vm((R, 1, DZ), F32), vm((R, 1, DZ), F32),
                vm((DZ, D), BF),
                vm((NQ, D, 2 * B), BF),
                vm((NQ, 2, R, B, B), BF),
                vm((R, B, D), BF),
                vm((R, 2 * B, DZ), BF),
                vm((DZ, B), BF),
                vm((R - 1, R, 2, B, B), F32),
                vm((R, 2, B, B), F32),
                vm((R, B, 2 * B), F32),
                vm((R, D, 2 * B), BF),
                vm((R, 2, R, B, B), F32),
                vm((R, R - 1, 2, B, B), F32),
                vm((R, B, 2 * B), BF),
                vm((R, B, DZ), BF),
                vm((B, D), BF),
                vm((R, 8, B, W), BF),
                sem((NSEND,)), sem((NRECV,)), sem((NLOC,)),
            ],
            compiler_params=pltpu.CompilerParams(
                collective_id=0, has_side_effects=True, vmem_limit_bytes=53 * 2**20),
            name="block",
        )(x.reshape(R, 2, R, B, B), g1.reshape(1, B), g2.reshape(1, B), w_gate, w_up, w_down, o, w_o, w_qkv)
        return pl.pallas_call(
            _copy,
            out_shape=(jax.ShapeDtypeStruct((D, B), BF), jax.ShapeDtypeStruct((D, W), BF)),
            in_specs=[pl.BlockSpec(memory_space=vm)] * 2,
            out_specs=(anyspec, anyspec),
            scratch_shapes=[sem((2, 4))],
            compiler_params=pltpu.CompilerParams(vmem_limit_bytes=2**20),
            name="store",
        )(*outs)

    h = ("z", "y", "c")
    in_specs = (P(None, h), P(h), P(h), P(h, "x"), P(h, "x"), P("x", h), P(None, "x"), P("x", h), P(h, "x"))
    return jax.shard_map(body, mesh=mesh4, in_specs=in_specs, out_specs=(P(None, h), P(None, "x")), check_vma=False)
```
